32 devices in a mesh: branch: 4 (over z), row: 4 (over y, core), col: 2 (over x).
Axes of the slice: x: 2, y: 2, z: 4, core: 2. Of those that a mesh axis runs over, the one named last changes fastest.
Arguments:
- homolog_tensor: bfloat16 [64, 128, 256], P('col', 'row'), may hold values from -6 to 6
- couple_tensor: bfloat16 [128, 128, 128], P('row', 'col'), may hold values from -6 to 6
- probe_matrix: bfloat16 [256, 256], P(None, 'branch'), may hold values from -0.375 to 0.375
- lookup_matrix: bfloat16 [256, 256], P(None, 'branch'), may hold values from -0.375 to 0.375
- content_matrix: bfloat16 [256, 256], P(None, 'branch'), may hold values from -0.375 to 0.375
- scoring_sigmoid_matrix: bfloat16 [256, 256], P(None, 'branch'), may hold values from -0.375 to 0.375
- scoring_final_matrix: bfloat16 [256, 256], P('branch'), may hold values from -0.375 to 0.375
- couple_offset_matrix: bfloat16 [128, 8], P(None, 'branch'), may hold values from -43 to 43
- product_first_matrix: bfloat16 [256, 32], replicated, may hold values from -0.375 to 0.375
- product_second_matrix: bfloat16 [256, 32], replicated, may hold values from -0.375 to 0.375
- product_final_matrix: bfloat16 [1024, 128], replicated, may hold values from -1 to 1
- trio_first_matrix: bfloat16 [2, 128, 128], P(None, None, 'branch'), may hold values from -0.5 to 0.5
- trio_second_matrix: bfloat16 [2, 128, 128], P(None, None, 'branch'), may hold values from -0.5 to 0.5
- trio_sigmoid_matrix: bfloat16 [128, 128], replicated, may hold values from -0.5 to 0.5
- trio_final_matrix: bfloat16 [128, 128], replicated, may hold values from -0.5 to 0.5
Outputs:
- revised_homolog_matrix: bfloat16 [64, 128, 256], P('col', 'row', 'branch')
- pairwise_output: bfloat16 [128, 128, 128], P('row', 'col')
The draws below stay inside these ranges and needn't reach their ends.
All inputs are finite; a program needn't handle non-finite values.
Results may differ from the reference program's by a relative error of at most 0.014.
Values may be sent and summed in bfloat16 or wider, within the bound.
No kernel may reach another device: no remote copies, remote signals or barrier semaphores. Data moves between devices by JAX's collectives and lax.ppermute only.
A program may use at most 64 MiB of HBM per device.

```python
import jax
import jax.numpy as jnp
from jax import lax

ROW_CHANNELS = 256
CP = 128
NUM_SUBSPACES = 8
SUBSPACE_SIZE = 32
PROJ_CHANNELS = 32
NUM_POSITIONS = 128
NUM_HOMOLOGS = 64


def draw_couple_offset_matrix(key, part):
    first, second = jax.random.split(jax.random.fold_in(key, 7))
    base = jnp.clip(jax.random.normal(first, (CP, NUM_SUBSPACES), jnp.float32), -4.0, 4.0) * 0.088
    scales = jax.random.uniform(second, (1, NUM_SUBSPACES), jnp.float32, 0.5, 2.0)
    return (base * scales).astype(jnp.bfloat16)


def block_scale(own_key, shape, shards, least, largest):
    def one(dim, shards_of):
        heights = jax.random.uniform(jax.random.fold_in(jax.random.fold_in(own_key, 6), dim), (shards_of,), jnp.float32, least / len(shards), largest / len(shards))
        return jnp.repeat(jnp.exp(heights), shape[dim] // shards_of).reshape((-1,) + (1,) * (len(shape) - dim - 1))

    gain = one(*shards[0])
    for cut in shards[1:]:
        gain = gain * one(*cut)
    return gain


def scatter_about(stream_key, shape, deviation, reach, shards=(), dtype=jnp.bfloat16):
    result = deviation * jax.random.normal(stream_key, shape, jnp.float32)
    if shards:
        result = result * block_scale(stream_key, shape, shards, -0.22, 0.18)
    return jnp.clip(result, -reach, reach).astype(dtype)


def setup_inputs(seed: int = 0) -> dict:
    splits = jax.random.split(jax.random.key(seed), 16)
    return {
        "homolog_tensor": scatter_about(splits[0], (NUM_HOMOLOGS, NUM_POSITIONS, ROW_CHANNELS), 1.0, 6.0, ((0, 2), (1, 4))),
        "couple_tensor": scatter_about(splits[1], (NUM_POSITIONS, NUM_POSITIONS, CP), 1.0, 6.0, ((0, 4), (1, 2))),
        "probe_matrix": scatter_about(splits[2], (ROW_CHANNELS, NUM_SUBSPACES * SUBSPACE_SIZE), ROW_CHANNELS ** -0.5, 0.375, ((1, 4),)),
        "lookup_matrix": scatter_about(splits[3], (ROW_CHANNELS, NUM_SUBSPACES * SUBSPACE_SIZE), ROW_CHANNELS ** -0.5, 0.375, ((1, 4),)),
        "content_matrix": scatter_about(splits[4], (ROW_CHANNELS, NUM_SUBSPACES * SUBSPACE_SIZE), ROW_CHANNELS ** -0.5, 0.375, ((1, 4),)),
        "scoring_sigmoid_matrix": scatter_about(splits[5], (ROW_CHANNELS, NUM_SUBSPACES * SUBSPACE_SIZE), ROW_CHANNELS ** -0.5, 0.375, ((1, 4),)),
        "scoring_final_matrix": scatter_about(splits[6], (NUM_SUBSPACES * SUBSPACE_SIZE, ROW_CHANNELS), (NUM_SUBSPACES * SUBSPACE_SIZE) ** -0.5, 0.375, ((0, 4),)),
        "couple_offset_matrix": draw_couple_offset_matrix(jax.random.fold_in(splits[15], 71), 0),
        "product_first_matrix": scatter_about(splits[8], (ROW_CHANNELS, PROJ_CHANNELS), ROW_CHANNELS ** -0.5, 0.375),
        "product_second_matrix": scatter_about(splits[9], (ROW_CHANNELS, PROJ_CHANNELS), ROW_CHANNELS ** -0.5, 0.375),
        "product_final_matrix": scatter_about(splits[10], (PROJ_CHANNELS * PROJ_CHANNELS, CP), PROJ_CHANNELS ** -0.5, 1.0),
        "trio_first_matrix": scatter_about(splits[11], (2, CP, CP), CP ** -0.5, 0.5, ((2, 4),)),
        "trio_second_matrix": scatter_about(splits[12], (2, CP, CP), CP ** -0.5, 0.5, ((2, 4),)),
        "trio_sigmoid_matrix": scatter_about(splits[13], (CP, CP), CP ** -0.5, 0.5),
        "trio_final_matrix": scatter_about(splits[14], (CP, CP), CP ** -0.5, 0.5),
    }


EPS = 1e-05

def standardise_rows(values):
    values = values.astype(jnp.float32)
    centred = values - lax.optimization_barrier(jnp.mean(values, axis=-1, keepdims=True))
    variance = lax.optimization_barrier(jnp.mean(centred * centred, axis=-1, keepdims=True))
    return centred / jnp.sqrt(variance + EPS)

def reference(homolog_tensor, couple_tensor, probe_matrix, lookup_matrix, content_matrix, scoring_sigmoid_matrix, scoring_final_matrix, couple_offset_matrix, product_first_matrix, product_second_matrix, product_final_matrix, trio_first_matrix, trio_second_matrix, trio_sigmoid_matrix, trio_final_matrix):
    standardised_tensor = standardise_rows(homolog_tensor).astype(jnp.bfloat16)
    reshaped_matrix = standardised_tensor.reshape(NUM_HOMOLOGS * NUM_POSITIONS, ROW_CHANNELS)

    def apply_linear(weights):
        return jnp.dot(reshaped_matrix, weights, preferred_element_type=jnp.float32)
    query = apply_linear(probe_matrix).astype(jnp.bfloat16).reshape(NUM_HOMOLOGS, NUM_POSITIONS, NUM_SUBSPACES, SUBSPACE_SIZE)
    key = apply_linear(lookup_matrix).astype(jnp.bfloat16).reshape(NUM_HOMOLOGS, NUM_POSITIONS, NUM_SUBSPACES, SUBSPACE_SIZE)
    value = apply_linear(content_matrix).astype(jnp.bfloat16).reshape(NUM_HOMOLOGS, NUM_POSITIONS, NUM_SUBSPACES, SUBSPACE_SIZE)
    gate_pre = apply_linear(scoring_sigmoid_matrix).reshape(NUM_HOMOLOGS, NUM_POSITIONS, NUM_SUBSPACES, SUBSPACE_SIZE)
    pair_normed = standardise_rows(couple_tensor).astype(jnp.bfloat16)
    pair_bias = jnp.dot(pair_normed.reshape(NUM_POSITIONS * NUM_POSITIONS, CP), couple_offset_matrix, preferred_element_type=jnp.float32)
    pair_bias = pair_bias.astype(jnp.bfloat16).reshape(NUM_POSITIONS, NUM_POSITIONS, NUM_SUBSPACES)
    bias_heads = jnp.transpose(pair_bias, (2, 0, 1)).astype(jnp.float32)
    scale = float(SUBSPACE_SIZE) ** (-0.5)

    def one_row(items):
        row_query, row_key, row_value = items
        scores = jnp.einsum('ihd,jhd->hij', row_query.astype(jnp.float32), row_key.astype(jnp.float32)) * scale
        scores = scores + bias_heads
        top = lax.optimization_barrier(jnp.max(scores, axis=-1, keepdims=True))
        expo = jnp.exp(scores - top)
        total = lax.optimization_barrier(jnp.sum(expo, axis=-1))
        weights = expo.astype(jnp.bfloat16)
        summed = jnp.einsum('hij,jhd->ihd', weights.astype(jnp.float32), row_value.astype(jnp.float32))
        return summed / jnp.transpose(total)[:, :, None]
    attended_values = lax.map(one_row, (query, key, value))
    attended_values = (attended_values * jax.nn.sigmoid(gate_pre)).astype(jnp.bfloat16)
    joined_tensor = jnp.dot(attended_values.reshape(NUM_HOMOLOGS * NUM_POSITIONS, NUM_SUBSPACES * SUBSPACE_SIZE), scoring_final_matrix, preferred_element_type=jnp.float32)
    revised_homolog_matrix = (homolog_tensor.astype(jnp.float32) + joined_tensor.reshape(NUM_HOMOLOGS, NUM_POSITIONS, ROW_CHANNELS)).astype(jnp.bfloat16)
    left_outer = apply_linear(product_first_matrix).astype(jnp.bfloat16).reshape(NUM_HOMOLOGS, NUM_POSITIONS, PROJ_CHANNELS)
    right_outer = apply_linear(product_second_matrix).astype(jnp.bfloat16).reshape(NUM_HOMOLOGS, NUM_POSITIONS, PROJ_CHANNELS)
    wide_out = product_final_matrix.astype(jnp.float32)

    def outer_block(piece):
        outer = jnp.einsum('sip,sjq->ijpq', piece.astype(jnp.float32), right_outer.astype(jnp.float32))
        return jnp.dot(outer.reshape(16 * NUM_POSITIONS, PROJ_CHANNELS * PROJ_CHANNELS), wide_out, precision=lax.Precision.HIGHEST).reshape(16, NUM_POSITIONS, CP)
    pieces = jnp.transpose(left_outer.reshape(NUM_HOMOLOGS, NUM_POSITIONS // 16, 16, PROJ_CHANNELS), (1, 0, 2, 3))
    outer_update = lax.map(outer_block, pieces).reshape(NUM_POSITIONS, NUM_POSITIONS, CP) / NUM_HOMOLOGS
    pair_mid = (couple_tensor.astype(jnp.float32) + outer_update).astype(jnp.bfloat16)
    tri_normed = standardise_rows(pair_mid).astype(jnp.bfloat16)
    tri_flat = tri_normed.reshape(NUM_POSITIONS * NUM_POSITIONS, CP)

    def gated(weights):
        linear = jnp.dot(tri_flat, weights[0], preferred_element_type=jnp.float32)
        opening = jnp.dot(tri_flat, weights[1], preferred_element_type=jnp.float32)
        return (jax.nn.sigmoid(opening) * linear).astype(jnp.bfloat16).reshape(NUM_POSITIONS, NUM_POSITIONS, CP)
    tri_left = gated(trio_first_matrix)
    tri_right = gated(trio_second_matrix)
    product = jnp.einsum('ikc,jkc->ijc', tri_left.astype(jnp.float32), tri_right.astype(jnp.float32))
    product_normed = standardise_rows(product).astype(jnp.bfloat16)
    closing = jax.nn.sigmoid(jnp.dot(tri_flat, trio_sigmoid_matrix, preferred_element_type=jnp.float32)).reshape(NUM_POSITIONS, NUM_POSITIONS, CP)
    change = jnp.dot(product_normed.reshape(NUM_POSITIONS * NUM_POSITIONS, CP), trio_final_matrix, preferred_element_type=jnp.float32).reshape(NUM_POSITIONS, NUM_POSITIONS, CP)
    pairwise_output = (pair_mid.astype(jnp.float32) + closing * change).astype(jnp.bfloat16)
    return (revised_homolog_matrix, pairwise_output)
```

```python
import functools

import jax
import jax.numpy as jnp
from jax import lax
from jax.experimental import pallas as pl
from jax.experimental.pallas import tpu as pltpu
from jax.sharding import PartitionSpec as P

EPS = 1e-05


def spread_2(block, axis, owner):
    block = jnp.where(lax.axis_index(axis) == owner, block, jnp.zeros_like(block))
    return lax.psum(block, axis)


def standardise_rows(values):
    values = values.astype(jnp.float32)
    centred = values - jnp.mean(values, axis=-1, keepdims=True)
    variance = jnp.mean(centred * centred, axis=-1, keepdims=True)
    return centred / jnp.sqrt(variance + EPS)


def apply_linear(source, weights):
    return jnp.dot(
        source.reshape(-1, weights.shape[0]), weights, preferred_element_type=jnp.float32
    )


def attend(query, key, value, bias):
    scale = float(query.shape[-1]) ** (-0.5)
    scores = jnp.einsum("sihd,sjhd->shij", query, key, preferred_element_type=jnp.float32) * scale
    scores = scores + jnp.transpose(bias, (2, 0, 1)).astype(jnp.float32)[None]
    top = jnp.max(scores, axis=-1, keepdims=True)
    expo = jnp.exp(scores - top)
    total = jnp.sum(expo, axis=-1)
    summed = jnp.einsum(
        "shij,sjhd->sihd", expo.astype(jnp.bfloat16), value, preferred_element_type=jnp.float32
    )
    return summed / jnp.transpose(total, (0, 2, 1))[..., None]


def plain_per_device(
    homolog_tensor,
    couple_tensor,
    probe_matrix,
    lookup_matrix,
    content_matrix,
    scoring_sigmoid_matrix,
    scoring_final_matrix,
    couple_offset_matrix,
    product_first_matrix,
    product_second_matrix,
    product_final_matrix,
    trio_first_matrix,
    trio_second_matrix,
    trio_sigmoid_matrix,
    trio_final_matrix,
):
    branches = lax.axis_size("branch")
    rows_count = lax.axis_size("row")
    cols_count = lax.axis_size("col")
    quadrant_share = lax.axis_index("branch")
    col_index = lax.axis_index("col")
    homolog_share, position_tile, channel_extent = homolog_tensor.shape
    c_block = couple_tensor.shape[1]
    residues = position_tile * rows_count
    depth = probe_matrix.shape[1]
    local_heads = couple_offset_matrix.shape[1]
    head_size = depth // local_heads
    q_rows = position_tile // branches
    total_rows = homolog_share * cols_count
    outer_width = product_first_matrix.shape[1]
    standardised_tensor = standardise_rows(homolog_tensor).astype(jnp.bfloat16)
    pair_normed = standardise_rows(couple_tensor).astype(jnp.bfloat16)
    bias_tile = (
        apply_linear(pair_normed, couple_offset_matrix)
        .astype(jnp.bfloat16)
        .reshape(position_tile, c_block, local_heads)
    )
    bias_band = lax.all_gather(bias_tile, "col", axis=1, tiled=True)
    spread = lax.all_to_all(standardised_tensor, "row", split_axis=0, concat_axis=1, tiled=True)
    few = spread.shape[0]
    shaped = (few, residues, local_heads, head_size)
    query = apply_linear(spread, probe_matrix).astype(jnp.bfloat16).reshape(shaped)
    key = apply_linear(spread, lookup_matrix).astype(jnp.bfloat16).reshape(shaped)
    value = apply_linear(spread, content_matrix).astype(jnp.bfloat16).reshape(shaped)
    gate_pre = apply_linear(spread, scoring_sigmoid_matrix).reshape(shaped)
    bias_full = lax.all_gather(bias_band, "row", axis=0, tiled=True)
    attended_values = attend(query, key, value, bias_full) * jax.nn.sigmoid(gate_pre)
    attended_values = attended_values.astype(jnp.bfloat16).reshape(few, residues, depth)
    attended_values = lax.all_to_all(
        attended_values, "row", split_axis=1, concat_axis=0, tiled=True
    )
    joined_tensor = apply_linear(attended_values, scoring_final_matrix).reshape(
        homolog_share, position_tile, channel_extent
    )
    joined_tensor = lax.psum_scatter(
        joined_tensor.astype(jnp.bfloat16), "branch", scatter_dimension=2, tiled=True
    ).astype(jnp.float32)
    device_share = channel_extent // branches
    local_alignment = lax.dynamic_slice_in_dim(
        homolog_tensor, quadrant_share * device_share, device_share, 2
    )
    revised_homolog_matrix = (local_alignment.astype(jnp.float32) + joined_tensor).astype(
        jnp.bfloat16
    )
    left_rows = lax.dynamic_slice_in_dim(standardised_tensor, quadrant_share * q_rows, q_rows, 1)
    left_outer = (
        apply_linear(left_rows, product_first_matrix)
        .astype(jnp.bfloat16)
        .reshape(homolog_share, q_rows * outer_width)
    )
    right_local = (
        apply_linear(standardised_tensor, product_second_matrix)
        .astype(jnp.bfloat16)
        .reshape(homolog_share, position_tile, outer_width)
    )
    right_outer = lax.all_gather(right_local, "row", axis=1, tiled=True)
    wide_out = product_final_matrix.astype(jnp.float32)
    left_major = jnp.transpose(left_outer)
    count = lax.axis_size("col") * c_block
    piece = right_outer.reshape(homolog_share, count * outer_width)
    outer = jnp.dot(left_major, piece, preferred_element_type=jnp.float32)
    outer = outer.reshape(q_rows, outer_width, count, outer_width)
    outer = jnp.transpose(outer, (2, 0, 1, 3)).reshape(count * q_rows, outer_width * outer_width)
    term = jnp.dot(outer, wide_out, precision=lax.Precision.HIGHEST) / total_rows
    update = lax.psum_scatter(
        term.reshape(count, q_rows, wide_out.shape[1]).astype(jnp.bfloat16),
        "col",
        scatter_dimension=0,
        tiled=True,
    ).astype(jnp.float32)
    update = jnp.transpose(update, (1, 0, 2))
    pair_rows = lax.dynamic_slice_in_dim(couple_tensor, quadrant_share * q_rows, q_rows, 0)
    mid_rows = (pair_rows.astype(jnp.float32) + update).astype(jnp.bfloat16)
    pair_mid = lax.all_gather(mid_rows, "branch", axis=0, tiled=True)
    tri_normed = standardise_rows(pair_mid).astype(jnp.bfloat16)

    def gated(weights):
        linear = apply_linear(tri_normed, weights[0])
        opening = apply_linear(tri_normed, weights[1])
        return (
            (jax.nn.sigmoid(opening) * linear)
            .astype(jnp.bfloat16)
            .reshape(position_tile, c_block, weights.shape[2])
        )

    tri_left = gated(trio_first_matrix)
    tri_right = gated(trio_second_matrix)
    left_band, right_band = (
        lax.all_gather(tri_left, "col", axis=1, tiled=True),
        lax.all_gather(tri_right, "col", axis=1, tiled=True),
    )
    ratio = rows_count // cols_count

    def mirror(offset):
        return spread_2(right_band, "row", col_index * ratio + offset)

    right_cols = jnp.concatenate([mirror(offset) for offset in range(ratio)], axis=0)
    product = jnp.einsum("ikc,jkc->ijc", left_band, right_cols, preferred_element_type=jnp.float32)
    product = lax.all_to_all(product, "branch", split_axis=0, concat_axis=2, tiled=True)
    product_normed = standardise_rows(product).astype(jnp.bfloat16)
    own_normed = lax.dynamic_slice_in_dim(tri_normed, quadrant_share * q_rows, q_rows, 0)
    closing = jax.nn.sigmoid(apply_linear(own_normed, trio_sigmoid_matrix)).reshape(
        q_rows, c_block, -1
    )
    change = apply_linear(product_normed, trio_final_matrix).reshape(q_rows, c_block, -1)
    out_rows = (mid_rows.astype(jnp.float32) + closing * change).astype(jnp.bfloat16)
    pairwise_output = lax.all_gather(out_rows, "branch", axis=0, tiled=True)
    return (revised_homolog_matrix, pairwise_output)


F32 = jnp.float32
BF16 = jnp.bfloat16
AXES = ("branch", "row", "col")
LANES = 128
HALF = LANES // 2
QUART = LANES // 4


def lane_of(shape):
    return lax.broadcasted_iota(jnp.int32, shape, len(shape) - 1)


def roll(x, shift):
    shift %= x.shape[-1]
    return pltpu.roll(x, shift, x.ndim - 1) if shift else x


def dot_nn(a, b):
    return jnp.dot(a, b, preferred_element_type=F32)


def dot_nt(a, b):
    return lax.dot_general(a, b, (((1,), (1,)), ((), ())), preferred_element_type=F32)


def call(body, outs, scratch=(), flops=0, n_in=None, name=None):
    return pl.pallas_call(
        body,
        out_shape=tuple(jax.ShapeDtypeStruct(s, d) for s, d in outs),
        scratch_shapes=[pltpu.VMEM(s, d) for s, d in scratch],
        compiler_params=pltpu.CompilerParams(vmem_limit_bytes=56 * 2**20),
        cost_estimate=pl.CostEstimate(flops=flops, bytes_accessed=2**19, transcendentals=0),
        name=name,
    )


def project_body(rows, hom, left_w, right_w, normed, left_t, right_t, scr):
    n_rows, depth = hom.shape
    share = n_rows // rows
    width = left_w.shape[1]
    step = 8
    for first in range(0, share, step):
        x = hom[first * rows : (first + step) * rows, :].astype(F32)
        x = x - jnp.mean(x, axis=-1, keepdims=True)
        x = x * lax.rsqrt(jnp.mean(x * x, axis=-1, keepdims=True) + EPS)
        normed[first * rows : (first + step) * rows, :] = x.astype(BF16)
        for s in range(step):
            piece = x[s * rows : (s + 1) * rows, :]
            for part in range(depth // LANES):
                scr[part, pl.ds(first + s, rows, stride=share), :] = piece[
                    :, part * LANES : (part + 1) * LANES
                ]
    w_l = jnp.transpose(left_w[...].astype(F32)).astype(BF16)
    w_r = jnp.transpose(right_w[...].astype(F32)).astype(BF16)
    weights = jnp.concatenate([w_l, w_r], axis=0)
    acc = 0
    for part in range(depth // LANES):
        acc = acc + dot_nt(
            weights[:, part * LANES : (part + 1) * LANES], scr[part].astype(BF16)
        )
    left_t[...] = acc[:width].astype(BF16)
    right_t[...] = acc[width:].astype(BF16)


def heads_body(normed, weights, kv, qg):
    depth = weights.shape[1] // 2
    full = dot_nn(normed[...], weights[...])
    kv[...] = full[:, :depth].astype(BF16)
    qg[...] = full[:, depth:]


def pair_body(local_heads, width, couple, offset_t, outer_w, couple_t, bias, outer_wt, scr, wscr):
    tiles = couple.shape[0] // LANES
    for t in range(tiles):
        x = jnp.transpose(couple[t * LANES : (t + 1) * LANES, :].astype(F32))
        couple_t[t] = x.astype(BF16)
        x = x - jnp.mean(x, axis=0, keepdims=True)
        x = x * lax.rsqrt(jnp.mean(x * x, axis=0, keepdims=True) + EPS)
        scr[pl.ds(t, offset_t.shape[0], stride=tiles), :] = dot_nn(offset_t[...], x.astype(BF16))
    bias[...] = scr[: local_heads * tiles, :].astype(BF16)
    wscr[...] = outer_w[...].astype(F32)
    per = LANES // width
    for g in range(width // per):
        block = jnp.concatenate(
            [wscr[pl.ds(g * per + q, width, stride=width), :] for q in range(per)], axis=0
        )
        outer_wt[:, g * LANES : (g + 1) * LANES] = jnp.transpose(block).astype(BF16)


def gate_pair(x, w_lin, w_open):
    return jax.nn.sigmoid(dot_nn(w_open, x)) * dot_nn(w_lin, x)


def store_gated(scr, t, rows, gated):
    chans = gated.shape[0] // 2
    low = lane_of((chans, LANES)) < HALF
    a, b = gated[:chans], gated[chans:]
    scr[pl.ds(2 * t, chans, stride=rows), :] = jnp.where(low, a, roll(b, HALF))
    scr[pl.ds(2 * t + 1, chans, stride=rows), :] = jnp.where(low, roll(a, HALF), b)


def outer_body(
    total_rows, couple_t, outer_wt, left_own, left_far, p_one, p_two, s_one, s_two, w_own, w_far,
    mid_t, norm_t, right_pk, lhs, rscr, mscr, gscr,
):
    col = lax.axis_index("col")
    row = lax.axis_index("row")
    chip_y, core = row // 2, row % 2
    width, span = left_own.shape
    tiles = couple_t.shape[0]
    rows = 2 * tiles
    share = span // rows
    block = rows * 2
    group = lane_of((width, LANES)) // share
    own_first = col == 0
    for g in range(span // LANES):
        cut = slice(g * LANES, (g + 1) * LANES)
        own, far = left_own[:, cut].astype(F32), left_far[:, cut].astype(F32)
        a, b = jnp.where(own_first, own, far), jnp.where(own_first, far, own)
        even = jnp.where(
            group == 0, a,
            jnp.where(group == 1, roll(b, QUART), jnp.where(group == 2, roll(a, QUART), roll(b, HALF))),
        )
        odd = jnp.where(
            group == 0, roll(a, HALF),
            jnp.where(group == 1, roll(b, -QUART), jnp.where(group == 2, roll(a, -QUART), b)),
        )
        lhs[2 * g * width : (2 * g + 1) * width, :] = even.astype(BF16)
        lhs[(2 * g + 1) * width : (2 * g + 2) * width, :] = odd.astype(BF16)
    first_one = chip_y == 0
    for a in range(2):
        mine = core == a
        for g in range(span // LANES):
            cut = slice(g * LANES, (g + 1) * LANES)
            one = jnp.where(mine, p_one[:, cut].astype(F32), s_one[:, cut].astype(F32))
            two = jnp.where(mine, p_two[:, cut].astype(F32), s_two[:, cut].astype(F32))
            t0, t1 = jnp.where(first_one, one, two), jnp.where(first_one, two, one)
            for j4 in range(LANES // share):
                j = a * rows + g * (LANES // share) + j4
                tile = jnp.where(
                    group == 0, roll(t0, -share * j4),
                    jnp.where(group == 1, roll(t1, share - share * j4), 0.0),
                )
                rscr[pl.ds(j, width, stride=2 * block), :] = tile
                rscr[pl.ds(block + j, width, stride=2 * block), :] = roll(tile, HALF)
    left = lhs[...]
    for q in range(0, width, 2):
        rhs = rscr[q * LANES : (q + 2) * LANES, :].astype(BF16)
        prod = dot_nt(left, rhs).astype(BF16)
        for t in range(tiles):
            for e in range(2):
                mscr[t, (q + e) * width : (q + e + 1) * width, :] = prod[
                    t * width : (t + 1) * width, e * LANES : (e + 1) * LANES
                ]
    w_lin = jnp.concatenate([w_own[2], w_far[2]], axis=0)
    w_open = jnp.concatenate([w_own[3], w_far[3]], axis=0)
    for t in range(0, tiles, 2):
        both = dot_nn(outer_wt[...], jnp.concatenate([mscr[t], mscr[t + 1]], axis=1))
        for e in range(2):
            update = both[:, e * LANES : (e + 1) * LANES] * (1.0 / total_rows)
            mid = (couple_t[t + e].astype(F32) + update).astype(BF16)
            mid_t[t + e] = mid
            x = mid.astype(F32)
            x = x - jnp.mean(x, axis=0, keepdims=True)
            x = x * lax.rsqrt(jnp.mean(x * x, axis=0, keepdims=True) + EPS)
            x = x.astype(BF16)
            norm_t[t + e] = x
            store_gated(gscr, t + e, rows, gate_pair(x, w_lin, w_open))
    right_pk[...] = gscr[...].astype(BF16)


def left_body(norm_t, w_own, w_far, close_w, left_pk, close_t, gscr):
    tiles = norm_t.shape[0]
    w_lin = jnp.concatenate([w_own[0], w_far[0]], axis=0)
    w_open = jnp.concatenate([w_own[1], w_far[1]], axis=0)
    w_close = jnp.transpose(close_w[...].astype(F32)).astype(BF16)
    for t in range(tiles):
        x = norm_t[t]
        store_gated(gscr, t, 2 * tiles, gate_pair(x, w_lin, w_open))
        close_t[t] = jax.nn.sigmoid(dot_nn(w_close, x))
    left_pk[...] = gscr[...].astype(BF16)


def triangle_body(rows, left_pk, own, sib, across, across_sib, mine, other):
    col = lax.axis_index("col")
    row = lax.axis_index("row")
    chip_y, core = row // 2, row % 2
    is_low, here = core == 0, chip_y == col
    low = lane_of((rows, LANES)) < HALF
    for ch in range(left_pk.shape[0] // rows):
        cut = slice(ch * rows, (ch + 1) * rows)
        a = left_pk[cut, :]
        zero = jnp.zeros_like(a)
        lhs = jnp.concatenate([jnp.where(low, a, zero), jnp.where(low, zero, a)], axis=0)
        o, s, x, xs = own[cut, :], sib[cut, :], across[cut, :], across_sib[cut, :]
        n0, n1 = jnp.where(is_low, o, s), jnp.where(is_low, s, o)
        f0, f1 = jnp.where(is_low, x, xs), jnp.where(is_low, xs, x)
        rhs = jnp.concatenate(
            [
                jnp.where(here, n0, f0), jnp.where(here, n1, f1),
                jnp.where(here, f0, n0), jnp.where(here, f1, n1),
            ],
            axis=0,
        )
        prod = dot_nt(lhs, rhs)
        u, v = prod[:rows], prod[rows:]
        mine[cut, :] = jnp.where(low, u, roll(v, HALF))
        other[cut, :] = jnp.where(low, roll(u, HALF), v).astype(BF16)


def final_body(rows, half_own, half_far, mid_t, close_t, final_w, out, scr, blocks):
    branch = lax.axis_index("branch")
    chans = half_own.shape[0] // rows
    count = 4 * chans
    low = lane_of((chans, LANES)) < HALF
    parts = [half_own[...].astype(F32), half_far[...].astype(F32)]
    parts = [p.reshape(chans, rows, LANES) for p in parts]
    total = jnp.sum(parts[0], axis=0) + jnp.sum(parts[1], axis=0)
    mean = (total + roll(total, HALF)) * (1.0 / count)
    parts = [p - mean[None] for p in parts]
    square = jnp.sum(parts[0] * parts[0], axis=0) + jnp.sum(parts[1] * parts[1], axis=0)
    scale = lax.rsqrt((square + roll(square, HALF)) * (1.0 / count) + EPS)
    for h in range(2):
        scr[h] = (parts[h] * scale[None]).reshape(chans * rows, LANES)
    w_t = jnp.transpose(final_w[...].astype(F32)).astype(BF16)
    owners = [branch, branch ^ 2, branch ^ 1, branch ^ 3]
    for t in range(rows // 2):
        for h in range(2):
            z0 = scr[h, pl.ds(2 * t, chans, stride=rows), :]
            z1 = scr[h, pl.ds(2 * t + 1, chans, stride=rows), :]
            first = jnp.where(low, z0, roll(z1, HALF))
            second = jnp.where(low, roll(z0, HALF), z1)
            for e, block in enumerate((first, second)):
                at = pl.multiple_of(owners[2 * h + e] * chans, chans)
                blocks[t % 2, pl.ds(at, chans), :] = block
        change = dot_nn(w_t, blocks[t % 2].astype(BF16))
        result = mid_t[t].astype(F32) + close_t[t] * change
        out[t * LANES : (t + 1) * LANES, :] = jnp.transpose(result).astype(BF16)


def attend_body(rows, head, qg, own, sib, across, across_sib, bias_own, bias_far, w_out, *rest):
    outs, (bscr, cscr) = rest[:-2], rest[-2:]
    col = lax.axis_index("col")
    row = lax.axis_index("row")
    branch = lax.axis_index("branch")
    chip_y, core = row // 2, row % 2
    is_low, top = core == 0, chip_y == 0
    share = qg.shape[0] // rows
    scale = float(head) ** (-0.5)
    b_own, b_far = bias_own[...].astype(F32), bias_far[...].astype(F32)
    b0, b1 = jnp.where(col == 0, b_own, b_far), jnp.where(col == 0, b_far, b_own)
    n_bias = b0.shape[0]
    low = lane_of((n_bias, LANES)) < HALF
    bscr[pl.ds(0, n_bias, stride=2), :] = jnp.where(low, b0, roll(b1, HALF))
    bscr[pl.ds(1, n_bias, stride=2), :] = jnp.where(low, roll(b0, HALF), b1)
    bias = bscr[...]
    lane = lane_of((rows, LANES))

    def one(s):
        cut = pl.ds(pl.multiple_of(s * rows, rows), rows)
        o, b, x, xs = own[cut, :], sib[cut, :], across[cut, :], across_sib[cut, :]
        n0, n1 = jnp.where(is_low, o, b), jnp.where(is_low, b, o)
        f0, f1 = jnp.where(is_low, x, xs), jnp.where(is_low, xs, x)
        kv = jnp.concatenate(
            [
                jnp.where(top, n0, f0), jnp.where(top, n1, f1),
                jnp.where(top, f0, n0), jnp.where(top, f1, n1),
            ],
            axis=0,
        )
        both = qg[cut, :]
        q = both.astype(BF16)
        zero = jnp.zeros_like(q)
        qm = jnp.concatenate(
            [
                jnp.where(lane < head, q, zero),
                jnp.where((lane >= head) & (lane < 2 * head), q, zero),
            ],
            axis=0,
        )
        scores = dot_nt(qm, kv) * scale + bias
        expo = jnp.exp(scores - jnp.max(scores, axis=-1, keepdims=True))
        total = jnp.sum(expo, axis=-1, keepdims=True)
        ctx = dot_nn(expo.astype(BF16), kv) / total
        ctx = jnp.where(lane < 3 * head, ctx[:rows], ctx[rows:])
        return ctx * jax.nn.sigmoid(both)

    half = share // 2

    def pair(s, carry):
        first, second = one(s), one(s + half)
        packed = jnp.where(lane < HALF, roll(first, HALF), second)
        cscr[pl.ds(pl.multiple_of(s * rows, rows), rows), :] = packed.astype(BF16)
        return carry

    lax.fori_loop(0, half, pair, 0, unroll=2)
    ctx = cscr[...]
    for m in range(len(outs)):
        outs[m][...] = dot_nn(ctx, w_out[branch ^ m]).astype(BF16)


def revise_body(hom, p0, p1, p2, p3, out):
    branch = lax.axis_index("branch")
    acc = p0[...].astype(F32) + p1[...].astype(F32)
    acc = acc + p2[...].astype(F32) + p3[...].astype(F32)
    n = acc.shape[0]
    at = pl.multiple_of((branch // 2) * LANES, LANES)
    base = hom[:, pl.ds(at, LANES)].astype(F32)
    base = jnp.where(branch % 2 == 0, base, roll(base, HALF))
    out[:n, :] = (acc + base[:n])[:, :HALF].astype(BF16)
    out[n:, :] = (roll(acc, HALF) + base[n:])[:, :HALF].astype(BF16)


def fast_per_device(
    mesh,
    homolog_tensor,
    couple_tensor,
    probe_matrix,
    lookup_matrix,
    content_matrix,
    scoring_sigmoid_matrix,
    scoring_final_matrix,
    couple_offset_matrix,
    product_first_matrix,
    product_second_matrix,
    product_final_matrix,
    trio_first_matrix,
    trio_second_matrix,
    trio_sigmoid_matrix,
    trio_final_matrix,
):
    n_b, n_r, n_c = (mesh.shape[a] for a in AXES)

    def send(x, source):
        pairs = []
        for b in range(n_b):
            for r in range(n_r):
                for c in range(n_c):
                    sb, sr, sc = source(b, r, c)
                    pairs.append(((sb * n_r + sr) * n_c + sc, (b * n_r + r) * n_c + c))
        return lax.ppermute(x, AXES, pairs)

    def other_col(b, r, c):
        return b, r, c ^ 1

    def other_core(b, r, c):
        return b, r ^ 1, c

    def other_chip(b, r, c):
        return b, r ^ 2, c

    def turned(b, r, c):
        return b, 2 * c + r % 2, r // 2

    def turned_far(b, r, c):
        return b, 2 * c + r % 2, (r // 2) ^ 1

    share, rows, depth = homolog_tensor.shape
    block = couple_tensor.shape[1]
    chans = couple_tensor.shape[2]
    width = product_first_matrix.shape[1]
    heads_w = probe_matrix.shape[1]
    local_heads = couple_offset_matrix.shape[1]
    head = heads_w // local_heads
    quarter = trio_first_matrix.shape[2]
    tiles = rows * block // LANES
    n_rows = share * rows
    hom = homolog_tensor.reshape(n_rows, depth)
    couple = couple_tensor.reshape(rows * block, chans)

    normed, left_t, right_t = call(
        functools.partial(project_body, rows),
        [((n_rows, depth), BF16), ((width, n_rows), BF16), ((width, n_rows), BF16)],
        [((depth // LANES, n_rows, LANES), F32)],
        name="project",
    )(hom, product_first_matrix, product_second_matrix)
    p_one = send(right_t, turned)
    p_two = send(right_t, turned_far)
    left_far = send(left_t, other_col)

    offset_t = jnp.pad(couple_offset_matrix.T, ((0, 8 - local_heads), (0, 0)))
    couple_t, bias, outer_wt = call(
        functools.partial(pair_body, local_heads, width),
        [
            ((tiles, chans, LANES), BF16),
            ((local_heads * tiles, LANES), BF16),
            ((chans, width * width), BF16),
        ],
        [((8 * tiles, LANES), F32), ((width * width, chans), F32)],
        name="pair",
    )(couple, offset_t, product_final_matrix)
    qkvg_w = jnp.concatenate(
        [lookup_matrix, content_matrix, probe_matrix, scoring_sigmoid_matrix], axis=1
    )
    kv, qg = call(
        heads_body, [((n_rows, 2 * heads_w), BF16), ((n_rows, 2 * heads_w), F32)], name="heads"
    )(normed, qkvg_w)
    w_own = jnp.transpose(
        jnp.concatenate([trio_first_matrix, trio_second_matrix], axis=0), (0, 2, 1)
    )
    w_far = send(w_own, lambda b, r, c: (b ^ 2, r, c))
    s_one, s_two = send(p_one, other_core), send(p_two, other_core)

    mid_t, norm_t, right_pk = call(
        functools.partial(outer_body, share * n_c),
        [
            ((tiles, chans, LANES), BF16),
            ((tiles, chans, LANES), BF16),
            ((quarter * rows, LANES), BF16),
        ],
        [
            ((tiles * width, LANES), BF16),
            ((width * LANES, LANES), F32),
            ((tiles, width * width, LANES), BF16),
            ((quarter * rows, LANES), F32),
        ],
        name="outer",
    )(couple_t, outer_wt, left_t, left_far, p_one, p_two, s_one, s_two, w_own, w_far)
    right_x = send(right_pk, other_chip)
    right_s = send(right_pk, other_core)
    left_pk, close_t = call(
        left_body,
        [((quarter * rows, LANES), BF16), ((tiles, chans, LANES), F32)],
        [((quarter * rows, LANES), F32)],
        name="left",
    )(norm_t, w_own, w_far, trio_sigmoid_matrix)
    right_xs = send(right_x, other_core)

    kv_x = send(kv, other_chip)
    bias_far = send(bias, other_col)
    kv_s = send(kv, other_core)
    kv_xs = send(kv_x, other_core)

    mine, other = call(
        functools.partial(triangle_body, rows),
        [((quarter * rows, LANES), F32), ((quarter * rows, LANES), BF16)],
        name="triangle",
    )(left_pk, right_pk, right_s, right_x, right_xs)
    far = send(other, other_col)
    half_own = (mine + far.astype(F32)).astype(BF16)
    half_far = send(half_own, lambda b, r, c: (b ^ 1, r, c))

    w4 = jnp.transpose(scoring_final_matrix.reshape(heads_w, n_b, depth // n_b), (1, 0, 2))
    zero = jnp.zeros_like(w4)
    w_out = jnp.concatenate(
        [jnp.concatenate([w4, zero], axis=2), jnp.concatenate([zero, w4], axis=2)], axis=1
    )
    parts = call(
        functools.partial(attend_body, rows, head),
        [((n_rows // 2, LANES), BF16)] * n_b,
        [((local_heads * rows, LANES), F32), ((n_rows // 2, LANES), BF16)],
        name="attend",
    )(qg, kv, kv_s, kv_x, kv_xs, bias, bias_far, w_out)
    parts = [parts[0]] + [
        send(parts[m], lambda b, r, c, m=m: (b ^ m, r, c)) for m in range(1, n_b)
    ]
    (revised,) = call(revise_body, [((n_rows, depth // n_b), BF16)], name="revise")(hom, *parts)

    (pair_out,) = call(
        functools.partial(final_body, rows),
        [((rows * block, chans), BF16)],
        [((2, quarter * rows, LANES), F32), ((2, chans, LANES), F32)],
        name="final",
    )(half_own, half_far, mid_t, close_t, trio_final_matrix)
    return (
        revised.reshape(share, rows, depth // n_b),
        pair_out.reshape(rows, block, chans),
    )


def fits(mesh, args):
    hom, couple = args[0], args[1]
    share, rows, depth = hom.shape
    return (
        mesh.shape["branch"] == 4
        and mesh.shape["row"] == 4
        and mesh.shape["col"] == 2
        and couple.shape[0] == rows
        and couple.shape[1] == 2 * rows == HALF
        and couple.shape[2] == LANES
        and share == QUART
        and args[2].shape[1] == HALF
        and depth == 4 * HALF
        and args[8].shape[1] == QUART
        and args[11].shape[2] == QUART
        and args[7].shape[1] == 2
    )


def dispatch(mesh, *args):
    if fits(mesh, args):
        return fast_per_device(mesh, *args)
    return plain_per_device(*args)


def solution(mesh):
    return jax.shard_map(
        functools.partial(dispatch, mesh),
        mesh=mesh,
        in_specs=(
            P("col", "row", None),
            P("row", "col", None),
            P(None, "branch"),
            P(None, "branch"),
            P(None, "branch"),
            P(None, "branch"),
            P("branch", None),
            P(None, "branch"),
            P(),
            P(),
            P(),
            P(None, None, "branch"),
            P(None, None, "branch"),
            P(),
            P(),
        ),
        out_specs=(P("col", "row", "branch"), P("row", "col", None)),
        check_vma=False,
    )
```

```python
import functools

import jax
import jax.numpy as jnp
from jax import lax
from jax.experimental import pallas as pl
from jax.experimental.pallas import tpu as pltpu
from jax.sharding import PartitionSpec as P


EPS = 1e-05


def spread_2(block, axis, owner):
    block = jnp.where(lax.axis_index(axis) == owner, block, jnp.zeros_like(block))
    return lax.psum(block, axis)


def standardise_rows(values):
    values = values.astype(jnp.float32)
    centred = values - jnp.mean(values, axis=-1, keepdims=True)
    variance = jnp.mean(centred * centred, axis=-1, keepdims=True)
    return centred / jnp.sqrt(variance + EPS)


def apply_linear(source, weights):
    return jnp.dot(
        source.reshape(-1, weights.shape[0]), weights, preferred_element_type=jnp.float32
    )


def attend(query, key, value, bias):
    scale = float(query.shape[-1]) ** (-0.5)
    scores = jnp.einsum("sihd,sjhd->shij", query, key, preferred_element_type=jnp.float32) * scale
    scores = scores + jnp.transpose(bias, (2, 0, 1)).astype(jnp.float32)[None]
    top = jnp.max(scores, axis=-1, keepdims=True)
    expo = jnp.exp(scores - top)
    total = jnp.sum(expo, axis=-1)
    summed = jnp.einsum(
        "shij,sjhd->sihd", expo.astype(jnp.bfloat16), value, preferred_element_type=jnp.float32
    )
    return summed / jnp.transpose(total, (0, 2, 1))[..., None]


def plain_per_device(
    homolog_tensor,
    couple_tensor,
    probe_matrix,
    lookup_matrix,
    content_matrix,
    scoring_sigmoid_matrix,
    scoring_final_matrix,
    couple_offset_matrix,
    product_first_matrix,
    product_second_matrix,
    product_final_matrix,
    trio_first_matrix,
    trio_second_matrix,
    trio_sigmoid_matrix,
    trio_final_matrix,
):
    branches = lax.axis_size("branch")
    rows_count = lax.axis_size("row")
    cols_count = lax.axis_size("col")
    quadrant_share = lax.axis_index("branch")
    col_index = lax.axis_index("col")
    homolog_share, position_tile, channel_extent = homolog_tensor.shape
    c_block = couple_tensor.shape[1]
    residues = position_tile * rows_count
    depth = probe_matrix.shape[1]
    local_heads = couple_offset_matrix.shape[1]
    head_size = depth // local_heads
    q_rows = position_tile // branches
    total_rows = homolog_share * cols_count
    outer_width = product_first_matrix.shape[1]
    standardised_tensor = standardise_rows(homolog_tensor).astype(jnp.bfloat16)
    pair_normed = standardise_rows(couple_tensor).astype(jnp.bfloat16)
    bias_tile = (
        apply_linear(pair_normed, couple_offset_matrix)
        .astype(jnp.bfloat16)
        .reshape(position_tile, c_block, local_heads)
    )
    bias_band = lax.all_gather(bias_tile, "col", axis=1, tiled=True)
    spread = lax.all_to_all(standardised_tensor, "row", split_axis=0, concat_axis=1, tiled=True)
    few = spread.shape[0]
    shaped = (few, residues, local_heads, head_size)
    query = apply_linear(spread, probe_matrix).astype(jnp.bfloat16).reshape(shaped)
    key = apply_linear(spread, lookup_matrix).astype(jnp.bfloat16).reshape(shaped)
    value = apply_linear(spread, content_matrix).astype(jnp.bfloat16).reshape(shaped)
    gate_pre = apply_linear(spread, scoring_sigmoid_matrix).reshape(shaped)
    bias_full = lax.all_gather(bias_band, "row", axis=0, tiled=True)
    attended_values = attend(query, key, value, bias_full) * jax.nn.sigmoid(gate_pre)
    attended_values = attended_values.astype(jnp.bfloat16).reshape(few, residues, depth)
    attended_values = lax.all_to_all(
        attended_values, "row", split_axis=1, concat_axis=0, tiled=True
    )
    joined_tensor = apply_linear(attended_values, scoring_final_matrix).reshape(
        homolog_share, position_tile, channel_extent
    )
    joined_tensor = lax.psum_scatter(
        joined_tensor.astype(jnp.bfloat16), "branch", scatter_dimension=2, tiled=True
    ).astype(jnp.float32)
    device_share = channel_extent // branches
    local_alignment = lax.dynamic_slice_in_dim(
        homolog_tensor, quadrant_share * device_share, device_share, 2
    )
    revised_homolog_matrix = (local_alignment.astype(jnp.float32) + joined_tensor).astype(
        jnp.bfloat16
    )
    left_rows = lax.dynamic_slice_in_dim(standardised_tensor, quadrant_share * q_rows, q_rows, 1)
    left_outer = (
        apply_linear(left_rows, product_first_matrix)
        .astype(jnp.bfloat16)
        .reshape(homolog_share, q_rows * outer_width)
    )
    right_local = (
        apply_linear(standardised_tensor, product_second_matrix)
        .astype(jnp.bfloat16)
        .reshape(homolog_share, position_tile, outer_width)
    )
    right_outer = lax.all_gather(right_local, "row", axis=1, tiled=True)
    wide_out = product_final_matrix.astype(jnp.float32)
    left_major = jnp.transpose(left_outer)
    count = lax.axis_size("col") * c_block
    piece = right_outer.reshape(homolog_share, count * outer_width)
    outer = jnp.dot(left_major, piece, preferred_element_type=jnp.float32)
    outer = outer.reshape(q_rows, outer_width, count, outer_width)
    outer = jnp.transpose(outer, (2, 0, 1, 3)).reshape(count * q_rows, outer_width * outer_width)
    term = jnp.dot(outer, wide_out, precision=lax.Precision.HIGHEST) / total_rows
    update = lax.psum_scatter(
        term.reshape(count, q_rows, wide_out.shape[1]).astype(jnp.bfloat16),
        "col",
        scatter_dimension=0,
        tiled=True,
    ).astype(jnp.float32)
    update = jnp.transpose(update, (1, 0, 2))
    pair_rows = lax.dynamic_slice_in_dim(couple_tensor, quadrant_share * q_rows, q_rows, 0)
    mid_rows = (pair_rows.astype(jnp.float32) + update).astype(jnp.bfloat16)
    pair_mid = lax.all_gather(mid_rows, "branch", axis=0, tiled=True)
    tri_normed = standardise_rows(pair_mid).astype(jnp.bfloat16)

    def gated(weights):
        linear = apply_linear(tri_normed, weights[0])
        opening = apply_linear(tri_normed, weights[1])
        return (
            (jax.nn.sigmoid(opening) * linear)
            .astype(jnp.bfloat16)
            .reshape(position_tile, c_block, weights.shape[2])
        )

    tri_left = gated(trio_first_matrix)
    tri_right = gated(trio_second_matrix)
    left_band, right_band = (
        lax.all_gather(tri_left, "col", axis=1, tiled=True),
        lax.all_gather(tri_right, "col", axis=1, tiled=True),
    )
    ratio = rows_count // cols_count

    def mirror(offset):
        return spread_2(right_band, "row", col_index * ratio + offset)

    right_cols = jnp.concatenate([mirror(offset) for offset in range(ratio)], axis=0)
    product = jnp.einsum("ikc,jkc->ijc", left_band, right_cols, preferred_element_type=jnp.float32)
    product = lax.all_to_all(product, "branch", split_axis=0, concat_axis=2, tiled=True)
    product_normed = standardise_rows(product).astype(jnp.bfloat16)
    own_normed = lax.dynamic_slice_in_dim(tri_normed, quadrant_share * q_rows, q_rows, 0)
    closing = jax.nn.sigmoid(apply_linear(own_normed, trio_sigmoid_matrix)).reshape(
        q_rows, c_block, -1
    )
    change = apply_linear(product_normed, trio_final_matrix).reshape(q_rows, c_block, -1)
    out_rows = (mid_rows.astype(jnp.float32) + closing * change).astype(jnp.bfloat16)
    pairwise_output = lax.all_gather(out_rows, "branch", axis=0, tiled=True)
    return (revised_homolog_matrix, pairwise_output)


F32 = jnp.float32
BF16 = jnp.bfloat16
AXES = ("branch", "row", "col")
LANES = 128
HALF = LANES // 2
QUART = LANES // 4


def lane_of(shape):
    return lax.broadcasted_iota(jnp.int32, shape, len(shape) - 1)


def roll(x, shift):
    shift %= x.shape[-1]
    return pltpu.roll(x, shift, x.ndim - 1) if shift else x


def dot_nn(a, b):
    return jnp.dot(a, b, preferred_element_type=F32)


def dot_nt(a, b):
    return lax.dot_general(a, b, (((1,), (1,)), ((), ())), preferred_element_type=F32)


def call(body, outs, scratch=(), flops=10**6, mib=8, sems=0, anywhere=0, out_hbm=0, alias=None):
    scratch = [pltpu.VMEM(s, d) for s, d in scratch]
    scratch += [pltpu.SemaphoreType.DMA] * sems
    far, near = pl.BlockSpec(memory_space=pltpu.HBM), pl.BlockSpec(memory_space=pltpu.VMEM)

    def run(*args):
        specs = {}
        if anywhere:
            specs["in_specs"] = [far] * anywhere + [near] * (len(args) - anywhere)
        if out_hbm:
            specs["out_specs"] = (far,) * out_hbm
        args = [
            pltpu.with_memory_space_constraint(x, pltpu.HBM) if n < anywhere else x
            for n, x in enumerate(args)
        ]
        return pl.pallas_call(
            body,
            out_shape=tuple(jax.ShapeDtypeStruct(s, d) for s, d in outs),
            scratch_shapes=scratch,
            compiler_params=pltpu.CompilerParams(vmem_limit_bytes=mib * 2**20),
            cost_estimate=pl.CostEstimate(flops=flops, bytes_accessed=2**19, transcendentals=0),
            input_output_aliases=alias or {},
            **specs,
        )(*args)

    return run


def project_body(
    rows, hom_h, left_h, right_h, couple_h, outer_h, offset_h, first_h, second_h,
    normed, left_t, right_t, couple, outer_w, offset, gates_w, scr, hom, left_w, right_w, *sems,
):
    parts = 2
    cut = hom.shape[0] // parts
    pieces = [pl.ds(n * cut, cut) for n in range(parts)]
    pairs = [(hom_h.at[p], hom.at[p]) for p in pieces]
    pairs += [(left_h, left_w), (right_h, right_w), (couple_h, couple), (outer_h, outer_w)]
    pairs += [(offset_h, offset), (first_h, gates_w.at[pl.ds(0, 2)])]
    pairs += [(second_h, gates_w.at[pl.ds(2, 2)])]
    moves = [pltpu.make_async_copy(src, dst, sem) for (src, dst), sem in zip(pairs, sems)]
    for move in moves[: parts + 2]:
        move.start()
    n_rows, depth = hom.shape
    share = n_rows // rows
    width = left_w.shape[0]
    step = 2
    for first in range(0, share, step):
        if first * rows % cut == 0:
            moves[first * rows // cut].wait()
        if first == 0:
            for move in moves[parts + 2 :]:
                move.start()
        x = hom[first * rows : (first + step) * rows, :].astype(F32)
        x = x - jnp.mean(x, axis=-1, keepdims=True)
        x = x * lax.rsqrt(jnp.mean(x * x, axis=-1, keepdims=True) + EPS)
        normed[first * rows : (first + step) * rows, :] = x.astype(BF16)
        for s in range(step):
            piece = x[s * rows : (s + 1) * rows, :]
            for part in range(depth // LANES):
                scr[part, pl.ds(first + s, rows, stride=share), :] = piece[
                    :, part * LANES : (part + 1) * LANES
                ]
    moves[parts].wait()
    moves[parts + 1].wait()
    weights = jnp.concatenate([left_w[...], right_w[...]], axis=0)
    acc = 0
    for part in range(depth // LANES):
        acc = acc + dot_nt(
            weights[:, part * LANES : (part + 1) * LANES], scr[part].astype(BF16)
        )
    for g in range(n_rows // LANES):
        cut = slice(g * LANES, (g + 1) * LANES)
        left_t[g * width : (g + 1) * width, :] = acc[:width, cut].astype(BF16)
        right_t[g * width : (g + 1) * width, :] = acc[width:, cut].astype(BF16)
    for move in moves[parts + 2 :]:
        move.wait()


def heads_body(normed, key_w, value_w, query_w, gate_w, kv, query, gate):
    half = normed.shape[0] // 2
    x = normed[...]
    low = lane_of((half, LANES)) < HALF

    def both(w0, w1):
        y = dot_nt(x, jnp.concatenate([w0[...], w1[...]], axis=0))
        top, bottom = y[:half], y[half:]
        return (
            jnp.where(low, top, roll(bottom, HALF)),
            jnp.where(low, roll(top, HALF), bottom),
        )

    k, v = both(key_w, value_w)
    kv[:half, :] = k.astype(BF16)
    kv[half:, :] = v.astype(BF16)
    q, g = both(query_w, gate_w)
    query[...] = q.astype(BF16)
    gate[...] = jax.nn.sigmoid(g)


def pair_body(width, couple, offset_t, outer_w, left_t, couple_t, message, outer_wt, scr, wscr):
    tiles = couple.shape[0] // LANES
    for t in range(tiles):
        x = jnp.transpose(couple[t * LANES : (t + 1) * LANES, :].astype(F32))
        couple_t[t] = x.astype(BF16)
        x = x - jnp.mean(x, axis=0, keepdims=True)
        x = x * lax.rsqrt(jnp.mean(x * x, axis=0, keepdims=True) + EPS)
        scr[pl.ds(t, offset_t.shape[0], stride=tiles), :] = dot_nn(offset_t[...], x.astype(BF16))
    span = left_t.shape[0]
    message[:span, :] = left_t[...]
    message[span:, :] = scr[...].astype(BF16)
    wscr[...] = outer_w[...].astype(F32)
    per = LANES // width
    for g in range(width // per):
        block = jnp.concatenate(
            [wscr[pl.ds(g * per + q, width, stride=width), :] for q in range(per)], axis=0
        )
        outer_wt[:, g * LANES : (g + 1) * LANES] = jnp.transpose(block).astype(BF16)


def gate_tiles(scr, norm_t, w_own, w_far, first):
    tiles = norm_t.shape[0]
    weights = jnp.concatenate(
        [w_own[first], w_far[first], w_own[first + 1], w_far[first + 1]], axis=0
    )
    half = weights.shape[0] // 2
    for t in range(0, tiles, 2):
        y = dot_nn(weights, jnp.concatenate([norm_t[t], norm_t[t + 1]], axis=1))
        gated = jax.nn.sigmoid(y[half:]) * y[:half]
        store_gated(scr, t, 2 * tiles, gated[:, :LANES])
        store_gated(scr, t + 1, 2 * tiles, gated[:, LANES:])


def store_gated(scr, t, rows, gated):
    chans = gated.shape[0] // 2
    low = lane_of((chans, LANES)) < HALF
    a, b = gated[:chans], gated[chans:]
    scr[pl.ds(2 * t, chans, stride=rows), :] = jnp.where(low, a, roll(b, HALF))
    scr[pl.ds(2 * t + 1, chans, stride=rows), :] = jnp.where(low, roll(a, HALF), b)


def outer_body(
    total_rows, couple_t, outer_wt, left_own, left_far, own_r, sib_r, got, got_sib,
    mid_t, norm_t, lhs, rscr, mscr,
):
    col = lax.axis_index("col")
    row = lax.axis_index("row")
    chip_y, core = row // 2, row % 2
    width = lhs.shape[0] // couple_t.shape[0]
    span = own_r.shape[0] // width * LANES
    tiles = couple_t.shape[0]
    rows = 2 * tiles
    share = span // rows
    block = rows * 2
    group = lane_of((width, LANES)) // share
    own_first = col == 0
    for g in range(span // LANES):
        cut = slice(g * width, (g + 1) * width)
        own, far = left_own[cut, :].astype(F32), left_far[cut, :].astype(F32)
        a, b = jnp.where(own_first, own, far), jnp.where(own_first, far, own)
        even = jnp.where(
            group == 0, a,
            jnp.where(group == 1, roll(b, QUART), jnp.where(group == 2, roll(a, QUART), roll(b, HALF))),
        )
        odd = jnp.where(
            group == 0, roll(a, HALF),
            jnp.where(group == 1, roll(b, -QUART), jnp.where(group == 2, roll(a, -QUART), b)),
        )
        lhs[2 * g * width : (2 * g + 1) * width, :] = even.astype(BF16)
        lhs[(2 * g + 1) * width : (2 * g + 2) * width, :] = odd.astype(BF16)
    here, north = chip_y == col, core == 0
    size = own_r.shape[0]
    for a in range(2):
        for g in range(span // LANES):
            cut = slice(g * width, (g + 1) * width)
            same = slice(a * size + g * width, a * size + (g + 1) * width)
            flip = slice((1 - a) * size + g * width, (1 - a) * size + (g + 1) * width)
            from_0 = jnp.where(north, got[same, :], got_sib[same, :])
            from_1 = jnp.where(north, got_sib[flip, :], got[flip, :])
            local = jnp.where(core == a, own_r[cut, :], sib_r[cut, :])
            one = jnp.where(here, local, from_0).astype(F32)
            two = jnp.where(here, from_0, from_1).astype(F32)
            t0, t1 = jnp.where(own_first, one, two), jnp.where(own_first, two, one)
            for j4 in range(LANES // share):
                j = a * rows + g * (LANES // share) + j4
                tile = jnp.where(
                    group == 0, roll(t0, -share * j4),
                    jnp.where(group == 1, roll(t1, share - share * j4), 0.0),
                )
                rscr[pl.ds(j, width, stride=2 * block), :] = tile
                rscr[pl.ds(block + j, width, stride=2 * block), :] = roll(tile, HALF)
    left = lhs[...]
    for q in range(0, width, 2):
        rhs = rscr[q * LANES : (q + 2) * LANES, :].astype(BF16)
        prod = dot_nt(left, rhs).astype(BF16)
        for t in range(tiles):
            for e in range(2):
                mscr[t, (q + e) * width : (q + e + 1) * width, :] = prod[
                    t * width : (t + 1) * width, e * LANES : (e + 1) * LANES
                ]
    for t in range(0, tiles, 2):
        both = dot_nn(outer_wt[...], jnp.concatenate([mscr[t], mscr[t + 1]], axis=1))
        for e in range(2):
            update = both[:, e * LANES : (e + 1) * LANES] * (1.0 / total_rows)
            mid = (couple_t[t + e].astype(F32) + update).astype(BF16)
            mid_t[t + e] = mid
            x = mid.astype(F32)
            x = x - jnp.mean(x, axis=0, keepdims=True)
            x = x * lax.rsqrt(jnp.mean(x * x, axis=0, keepdims=True) + EPS)
            norm_t[t + e] = x.astype(BF16)


def right_body(norm_t, w_own, w_far, right_pk, gscr):
    gate_tiles(gscr, norm_t, w_own, w_far, 2)
    right_pk[...] = gscr[...].astype(BF16)


def left_body(norm_t, w_own, w_far, left_pk, gscr):
    gate_tiles(gscr, norm_t, w_own, w_far, 0)
    left_pk[...] = gscr[...].astype(BF16)


def close_body(norm_t, close_w, close_t):
    w_close = jnp.transpose(close_w[...].astype(F32)).astype(BF16)
    for t in range(norm_t.shape[0]):
        close_t[t] = jax.nn.sigmoid(dot_nn(w_close, norm_t[t]))


def triangle_body(rows, part, left_pk, own, sib, across, across_sib, mine, other):
    col = lax.axis_index("col")
    row = lax.axis_index("row")
    chip_y, core = row // 2, row % 2
    is_low, here = core == 0, chip_y == col
    n = rows // 2
    low = lane_of((n, LANES)) < HALF
    for ch in range(left_pk.shape[0] // rows):
        cut = slice(ch * rows, (ch + 1) * rows)
        a = left_pk[ch * rows + part * n : ch * rows + (part + 1) * n, :]
        zero = jnp.zeros_like(a)
        lhs = jnp.concatenate([jnp.where(low, a, zero), jnp.where(low, zero, a)], axis=0)
        o, s, x, xs = own[cut, :], sib[cut, :], across[cut, :], across_sib[cut, :]
        n0, n1 = jnp.where(is_low, o, s), jnp.where(is_low, s, o)
        f0, f1 = jnp.where(is_low, x, xs), jnp.where(is_low, xs, x)
        rhs = jnp.concatenate(
            [
                jnp.where(here, n0, f0), jnp.where(here, n1, f1),
                jnp.where(here, f0, n0), jnp.where(here, f1, n1),
            ],
            axis=0,
        )
        prod = dot_nt(lhs, rhs)
        u, v = prod[:n], prod[n:]
        to = slice(ch * n, (ch + 1) * n)
        mine[to, :] = jnp.where(low, u, roll(v, HALF))
        other[to, :] = jnp.where(low, roll(u, HALF), v).astype(BF16)


def final_body(n, part, *refs):
    half_own, half_far, mid_t, close_t, final_w, out_h, scr, out, *sems = refs[part:]
    branch = lax.axis_index("branch")
    chans = half_own.shape[0] // n
    low = lane_of((chans, LANES)) < HALF
    scr[0] = half_own[...].astype(F32)
    scr[1] = half_far[...].astype(F32)
    owners = [branch, branch ^ 2, branch ^ 1, branch ^ 3]
    w_t = [final_w[pl.ds(pl.multiple_of(o * chans, chans), chans), :] for o in owners]
    w_t = jnp.transpose(jnp.concatenate(w_t, axis=0).astype(F32)).astype(BF16)
    tiles = n // 2
    per = tiles // len(sems)
    base = part * tiles
    moves = []
    for t in range(tiles):
        blocks = []
        for h in range(2):
            z0 = scr[h, pl.ds(2 * t, chans, stride=n), :]
            z1 = scr[h, pl.ds(2 * t + 1, chans, stride=n), :]
            blocks += [jnp.where(low, z0, roll(z1, HALF)), jnp.where(low, roll(z0, HALF), z1)]
        x = jnp.concatenate(blocks, axis=0)
        x = x - jnp.mean(x, axis=0, keepdims=True)
        x = x * lax.rsqrt(jnp.mean(x * x, axis=0, keepdims=True) + EPS)
        change = dot_nn(w_t, x.astype(BF16))
        result = mid_t[base + t].astype(F32) + close_t[base + t] * change
        out[t * LANES : (t + 1) * LANES, :] = jnp.transpose(result).astype(BF16)
        if t % per == per - 1:
            here = out.at[pl.ds((t + 1 - per) * LANES, per * LANES)]
            there = out_h.at[pl.ds((base + t + 1 - per) * LANES, per * LANES)]
            moves.append(pltpu.make_async_copy(here, there, sems[t // per]))
            moves[-1].start()
    for move in moves:
        move.wait()


def attend_body(
    rows, head, query, gate, own, sib, across, across_sib, sent, got, w_out, *rest
):
    outs, (bscr, cscr) = rest[:-2], rest[-2:]
    col = lax.axis_index("col")
    row = lax.axis_index("row")
    branch = lax.axis_index("branch")
    top, is_low = row // 2 == 0, row % 2 == 0
    half = query.shape[0]
    scale = float(head) ** (-0.5)
    n_bias = bscr.shape[0] // 2
    start = sent.shape[0] - n_bias
    b_own, b_far = sent[start:, :].astype(F32), got[start:, :].astype(F32)
    b0, b1 = jnp.where(col == 0, b_own, b_far), jnp.where(col == 0, b_far, b_own)
    low = lane_of((n_bias, LANES)) < HALF
    bscr[pl.ds(0, n_bias, stride=2), :] = jnp.where(low, b0, roll(b1, HALF))
    bscr[pl.ds(1, n_bias, stride=2), :] = jnp.where(low, roll(b0, HALF), b1)
    bias = jnp.transpose(jnp.concatenate([bscr[...], bscr[...]], axis=0))
    b = [bias[n * rows : (n + 1) * rows] for n in range(LANES // rows)]
    b = [jnp.where(is_low, b[n], b[n ^ 1]) for n in range(len(b))]
    b = [jnp.where(top, b[n], b[n ^ 2]) for n in range(len(b))]
    bias = jnp.concatenate(b, axis=0)
    group = lane_of((rows, LANES)) // head

    def gather(at):
        cut = pl.ds(pl.multiple_of(at, rows), rows)
        return jnp.concatenate([own[cut, :], sib[cut, :], across[cut, :], across_sib[cut, :]], axis=0)

    batch = 4

    def some(step, carry):
        spots = [(step * batch + n) * rows for n in range(batch)]
        cuts = [pl.ds(pl.multiple_of(at, rows), rows) for at in spots]
        masked = []
        for cut in cuts:
            q = query[cut, :]
            zero = jnp.zeros_like(q)
            masked.append(
                jnp.concatenate(
                    [jnp.where(group == g, q, zero) for g in range(LANES // head)], axis=0
                )
            )
        scores = [dot_nt(gather(at), q) * scale + bias for at, q in zip(spots, masked)]
        tops = [jnp.max(x, axis=0, keepdims=True) for x in scores]
        expo = [jnp.exp(x - top) for x, top in zip(scores, tops)]
        expo = [x * (1.0 / jnp.sum(x, axis=0, keepdims=True)) for x in expo]
        full = [
            lax.dot_general(
                x.astype(BF16), gather(half + at), (((0,), (0,)), ((), ())),
                preferred_element_type=F32,
            )
            for x, at in zip(expo, spots)
        ]
        for cut, x in zip(cuts, full):
            ctx = x[:rows]
            for g in range(1, LANES // head):
                ctx = jnp.where(group == g, x[g * rows : (g + 1) * rows], ctx)
            cscr[cut, :] = (ctx * gate[cut, :]).astype(BF16)
        return carry

    lax.fori_loop(0, half // rows // batch, some, 0, unroll=True)
    ctx = cscr[...]
    low = lane_of((w_out.shape[0], LANES)) < HALF
    for m in range(len(outs)):
        chunk = branch ^ m
        at = pl.multiple_of((chunk // 2) * LANES, LANES)
        w = w_out[:, pl.ds(at, LANES)].astype(F32)
        w = jnp.where(chunk % 2 == 0, w, roll(w, HALF))
        w = jnp.concatenate([jnp.where(low, w, 0.0), jnp.where(low, 0.0, roll(w, HALF))], axis=0)
        outs[m][...] = dot_nn(ctx, w.astype(BF16)).astype(BF16)


def revise_body(hom, p0, p1, p2, p3, out):
    branch = lax.axis_index("branch")
    acc = p0[...].astype(F32) + p1[...].astype(F32)
    acc = acc + p2[...].astype(F32) + p3[...].astype(F32)
    n = acc.shape[0]
    at = pl.multiple_of((branch // 2) * LANES, LANES)
    base = hom[:, pl.ds(at, LANES)].astype(F32)
    base = jnp.where(branch % 2 == 0, base, roll(base, HALF))
    out[:n, :] = (acc + base[:n])[:, :HALF].astype(BF16)
    out[n:, :] = (roll(acc, HALF) + base[n:])[:, :HALF].astype(BF16)


def fast_per_device(
    mesh,
    homolog_tensor,
    couple_tensor,
    probe_matrix,
    lookup_matrix,
    content_matrix,
    scoring_sigmoid_matrix,
    scoring_final_matrix,
    couple_offset_matrix,
    product_first_matrix,
    product_second_matrix,
    product_final_matrix,
    trio_first_matrix,
    trio_second_matrix,
    trio_sigmoid_matrix,
    trio_final_matrix,
):
    n_b, n_r, n_c = (mesh.shape[a] for a in AXES)

    def send(x, source):
        pairs = []
        for b in range(n_b):
            for r in range(n_r):
                for c in range(n_c):
                    if (origin := source(b, r, c)) is not None:
                        sb, sr, sc = origin
                        pairs.append(((sb * n_r + sr) * n_c + sc, (b * n_r + r) * n_c + c))
        return lax.ppermute(x, AXES, pairs)

    def other_col(b, r, c):
        return b, r, c ^ 1

    def other_core(b, r, c):
        return b, r ^ 1, c

    def other_chip(b, r, c):
        return b, r ^ 2, c

    def turned(b, r, c):
        y, core = r // 2, r % 2
        if y == c:
            return None if core else (b, r, c ^ 1)
        return b, 2 * c + core, c ^ core

    share, rows, depth = homolog_tensor.shape
    block = couple_tensor.shape[1]
    chans = couple_tensor.shape[2]
    width = product_first_matrix.shape[1]
    heads_w = probe_matrix.shape[1]
    local_heads = couple_offset_matrix.shape[1]
    head = heads_w // local_heads
    quarter = trio_first_matrix.shape[2]
    tiles = rows * block // LANES
    n_rows = share * rows
    hom = homolog_tensor.reshape(n_rows, depth)
    couple = couple_tensor.reshape(rows * block, chans)

    flat = (n_rows * width // LANES, LANES)
    normed, left_t, right_t, couple_v, outer_w, offset_t, w_own = call(
        functools.partial(project_body, rows),
        [
            ((n_rows, depth), BF16), (flat, BF16), (flat, BF16),
            (couple.shape, BF16), (product_final_matrix.shape, BF16),
            ((local_heads, chans), BF16), ((4, quarter, chans), BF16),
        ],
        [
            ((depth // LANES, n_rows, LANES), F32), ((n_rows, depth), BF16),
            ((width, depth), BF16), ((width, depth), BF16),
        ],
        sems=9,
        anywhere=8,
    )(
        hom, product_first_matrix.T, product_second_matrix.T, couple, product_final_matrix,
        couple_offset_matrix.T, jnp.transpose(trio_first_matrix, (0, 2, 1)),
        jnp.transpose(trio_second_matrix, (0, 2, 1)),
    )
    sib_r = send(right_t, other_core)
    got_r = send(jnp.concatenate([right_t, sib_r], axis=0), turned)
    couple_t, message, outer_wt = call(
        functools.partial(pair_body, width),
        [
            ((tiles, chans, LANES), BF16),
            ((flat[0] + local_heads * tiles, LANES), BF16),
            ((chans, width * width), BF16),
        ],
        [((local_heads * tiles, LANES), F32), ((width * width, chans), F32)],
    )(couple_v, offset_t, outer_w, left_t)
    got = send(message, other_col)
    kv, query, gate = call(
        heads_body,
        [((n_rows, LANES), BF16), ((n_rows // 2, LANES), BF16), ((n_rows // 2, LANES), F32)],
    )(normed, lookup_matrix.T, content_matrix.T, probe_matrix.T, scoring_sigmoid_matrix.T)
    kv_x = send(kv, other_chip)
    kv_s = send(kv, other_core)
    kv_xs = send(kv_x, other_core)
    w_far = send(w_own, lambda b, r, c: (b ^ 2, r, c))
    got_rs = send(got_r, other_core)

    mid_t, norm_t = call(
        functools.partial(outer_body, share * n_c),
        [((tiles, chans, LANES), BF16), ((tiles, chans, LANES), BF16)],
        [
            ((tiles * width, LANES), BF16),
            ((width * LANES, LANES), F32),
            ((tiles, width * width, LANES), BF16),
        ],
        mib=16,
    )(couple_t, outer_wt, message, got, right_t, sib_r, got_r, got_rs)
    (right_pk,) = call(
        right_body, [((quarter * rows, LANES), BF16)], [((quarter * rows, LANES), F32)]
    )(norm_t, w_own, w_far)
    right_x = send(right_pk, other_chip)
    right_s = send(right_pk, other_core)
    (left_pk,) = call(
        left_body, [((quarter * rows, LANES), BF16)], [((quarter * rows, LANES), F32)]
    )(norm_t, w_own, w_far)
    parts = call(
        functools.partial(attend_body, rows, head),
        [((n_rows // 2, LANES), BF16)] * n_b,
        [((local_heads * rows, LANES), F32), ((n_rows // 2, LANES), BF16)],
    )(query, gate, kv, kv_s, kv_x, kv_xs, message, got, scoring_final_matrix)
    right_xs = send(right_x, other_core)

    mines, fars = [], []
    for part in range(2):
        mine, other = call(
            functools.partial(triangle_body, rows, part),
            [((quarter * rows // 2, LANES), F32), ((quarter * rows // 2, LANES), BF16)],
        )(left_pk, right_pk, right_s, right_x, right_xs)
        mines.append(mine)
        fars.append(send(other, other_col))
    (close_t,) = call(close_body, [((tiles, chans, LANES), F32)])(norm_t, trio_sigmoid_matrix)
    parts = [parts[0]] + [send(parts[m], lambda b, r, c, m=m: (b ^ m, r, c)) for m in range(1, n_b)]
    half_own = [(mine + far.astype(F32)).astype(BF16) for mine, far in zip(mines, fars)]
    half_far = [send(half, lambda b, r, c: (b ^ 1, r, c)) for half in half_own]
    (revised,) = call(revise_body, [((n_rows, depth // n_b), BF16)])(hom, *parts)

    pair_out = ()
    for part in range(2):
        pair_out = call(
            functools.partial(final_body, rows // 2, part),
            [((rows * block, chans), BF16)],
            [((2, quarter * rows // 2, LANES), F32), ((rows * block // 2, chans), BF16)],
            mib=12,
            sems=2,
            out_hbm=1,
            anywhere=part,
            alias={0: 0} if part else None,
        )(*pair_out, half_own[part], half_far[part], mid_t, close_t, trio_final_matrix)
    (pair_out,) = pair_out
    return (
        revised.reshape(share, rows, depth // n_b),
        pair_out.reshape(rows, block, chans),
    )


def fits(mesh, args):
    hom, couple = args[0], args[1]
    share, rows, depth = hom.shape
    return (
        mesh.shape["branch"] == 4
        and mesh.shape["row"] == 4
        and mesh.shape["col"] == 2
        and couple.shape[0] == rows
        and couple.shape[1] == 2 * rows == HALF
        and couple.shape[2] == LANES
        and share == QUART
        and args[2].shape[1] == HALF
        and depth == 4 * HALF
        and args[8].shape[1] == QUART
        and args[11].shape[2] == QUART
        and args[7].shape[1] == 2
    )


def dispatch(mesh, *args):
    if fits(mesh, args):
        return fast_per_device(mesh, *args)
    return plain_per_device(*args)


def solution(mesh):
    return jax.shard_map(
        functools.partial(dispatch, mesh),
        mesh=mesh,
        in_specs=(
            P("col", "row", None),
            P("row", "col", None),
            P(None, "branch"),
            P(None, "branch"),
            P(None, "branch"),
            P(None, "branch"),
            P("branch", None),
            P(None, "branch"),
            P(),
            P(),
            P(),
            P(None, None, "branch"),
            P(None, None, "branch"),
            P(),
            P(),
        ),
        out_specs=(P("col", "row", "branch"), P("row", "col", None)),
        check_vma=False,
    )
```

```python
import functools

import jax
import jax.numpy as jnp
from jax import lax
from jax.experimental import pallas as pl
from jax.experimental.pallas import tpu as pltpu
from jax.sharding import PartitionSpec as P


EPS = 1e-05


def spread_2(block, axis, owner):
    block = jnp.where(lax.axis_index(axis) == owner, block, jnp.zeros_like(block))
    return lax.psum(block, axis)


def standardise_rows(values):
    values = values.astype(jnp.float32)
    centred = values - jnp.mean(values, axis=-1, keepdims=True)
    variance = jnp.mean(centred * centred, axis=-1, keepdims=True)
    return centred / jnp.sqrt(variance + EPS)


def apply_linear(source, weights):
    return jnp.dot(
        source.reshape(-1, weights.shape[0]), weights, preferred_element_type=jnp.float32
    )


def attend(query, key, value, bias):
    scale = float(query.shape[-1]) ** (-0.5)
    scores = jnp.einsum("sihd,sjhd->shij", query, key, preferred_element_type=jnp.float32) * scale
    scores = scores + jnp.transpose(bias, (2, 0, 1)).astype(jnp.float32)[None]
    top = jnp.max(scores, axis=-1, keepdims=True)
    expo = jnp.exp(scores - top)
    total = jnp.sum(expo, axis=-1)
    summed = jnp.einsum(
        "shij,sjhd->sihd", expo.astype(jnp.bfloat16), value, preferred_element_type=jnp.float32
    )
    return summed / jnp.transpose(total, (0, 2, 1))[..., None]


def plain_per_device(
    homolog_tensor,
    couple_tensor,
    probe_matrix,
    lookup_matrix,
    content_matrix,
    scoring_sigmoid_matrix,
    scoring_final_matrix,
    couple_offset_matrix,
    product_first_matrix,
    product_second_matrix,
    product_final_matrix,
    trio_first_matrix,
    trio_second_matrix,
    trio_sigmoid_matrix,
    trio_final_matrix,
):
    branches = lax.axis_size("branch")
    rows_count = lax.axis_size("row")
    cols_count = lax.axis_size("col")
    quadrant_share = lax.axis_index("branch")
    col_index = lax.axis_index("col")
    homolog_share, position_tile, channel_extent = homolog_tensor.shape
    c_block = couple_tensor.shape[1]
    residues = position_tile * rows_count
    depth = probe_matrix.shape[1]
    local_heads = couple_offset_matrix.shape[1]
    head_size = depth // local_heads
    q_rows = position_tile // branches
    total_rows = homolog_share * cols_count
    outer_width = product_first_matrix.shape[1]
    standardised_tensor = standardise_rows(homolog_tensor).astype(jnp.bfloat16)
    pair_normed = standardise_rows(couple_tensor).astype(jnp.bfloat16)
    bias_tile = (
        apply_linear(pair_normed, couple_offset_matrix)
        .astype(jnp.bfloat16)
        .reshape(position_tile, c_block, local_heads)
    )
    bias_band = lax.all_gather(bias_tile, "col", axis=1, tiled=True)
    spread = lax.all_to_all(standardised_tensor, "row", split_axis=0, concat_axis=1, tiled=True)
    few = spread.shape[0]
    shaped = (few, residues, local_heads, head_size)
    query = apply_linear(spread, probe_matrix).astype(jnp.bfloat16).reshape(shaped)
    key = apply_linear(spread, lookup_matrix).astype(jnp.bfloat16).reshape(shaped)
    value = apply_linear(spread, content_matrix).astype(jnp.bfloat16).reshape(shaped)
    gate_pre = apply_linear(spread, scoring_sigmoid_matrix).reshape(shaped)
    bias_full = lax.all_gather(bias_band, "row", axis=0, tiled=True)
    attended_values = attend(query, key, value, bias_full) * jax.nn.sigmoid(gate_pre)
    attended_values = attended_values.astype(jnp.bfloat16).reshape(few, residues, depth)
    attended_values = lax.all_to_all(
        attended_values, "row", split_axis=1, concat_axis=0, tiled=True
    )
    joined_tensor = apply_linear(attended_values, scoring_final_matrix).reshape(
        homolog_share, position_tile, channel_extent
    )
    joined_tensor = lax.psum_scatter(
        joined_tensor.astype(jnp.bfloat16), "branch", scatter_dimension=2, tiled=True
    ).astype(jnp.float32)
    device_share = channel_extent // branches
    local_alignment = lax.dynamic_slice_in_dim(
        homolog_tensor, quadrant_share * device_share, device_share, 2
    )
    revised_homolog_matrix = (local_alignment.astype(jnp.float32) + joined_tensor).astype(
        jnp.bfloat16
    )
    left_rows = lax.dynamic_slice_in_dim(standardised_tensor, quadrant_share * q_rows, q_rows, 1)
    left_outer = (
        apply_linear(left_rows, product_first_matrix)
        .astype(jnp.bfloat16)
        .reshape(homolog_share, q_rows * outer_width)
    )
    right_local = (
        apply_linear(standardised_tensor, product_second_matrix)
        .astype(jnp.bfloat16)
        .reshape(homolog_share, position_tile, outer_width)
    )
    right_outer = lax.all_gather(right_local, "row", axis=1, tiled=True)
    wide_out = product_final_matrix.astype(jnp.float32)
    left_major = jnp.transpose(left_outer)
    count = lax.axis_size("col") * c_block
    piece = right_outer.reshape(homolog_share, count * outer_width)
    outer = jnp.dot(left_major, piece, preferred_element_type=jnp.float32)
    outer = outer.reshape(q_rows, outer_width, count, outer_width)
    outer = jnp.transpose(outer, (2, 0, 1, 3)).reshape(count * q_rows, outer_width * outer_width)
    term = jnp.dot(outer, wide_out, precision=lax.Precision.HIGHEST) / total_rows
    update = lax.psum_scatter(
        term.reshape(count, q_rows, wide_out.shape[1]).astype(jnp.bfloat16),
        "col",
        scatter_dimension=0,
        tiled=True,
    ).astype(jnp.float32)
    update = jnp.transpose(update, (1, 0, 2))
    pair_rows = lax.dynamic_slice_in_dim(couple_tensor, quadrant_share * q_rows, q_rows, 0)
    mid_rows = (pair_rows.astype(jnp.float32) + update).astype(jnp.bfloat16)
    pair_mid = lax.all_gather(mid_rows, "branch", axis=0, tiled=True)
    tri_normed = standardise_rows(pair_mid).astype(jnp.bfloat16)

    def gated(weights):
        linear = apply_linear(tri_normed, weights[0])
        opening = apply_linear(tri_normed, weights[1])
        return (
            (jax.nn.sigmoid(opening) * linear)
            .astype(jnp.bfloat16)
            .reshape(position_tile, c_block, weights.shape[2])
        )

    tri_left = gated(trio_first_matrix)
    tri_right = gated(trio_second_matrix)
    left_band, right_band = (
        lax.all_gather(tri_left, "col", axis=1, tiled=True),
        lax.all_gather(tri_right, "col", axis=1, tiled=True),
    )
    ratio = rows_count // cols_count

    def mirror(offset):
        return spread_2(right_band, "row", col_index * ratio + offset)

    right_cols = jnp.concatenate([mirror(offset) for offset in range(ratio)], axis=0)
    product = jnp.einsum("ikc,jkc->ijc", left_band, right_cols, preferred_element_type=jnp.float32)
    product = lax.all_to_all(product, "branch", split_axis=0, concat_axis=2, tiled=True)
    product_normed = standardise_rows(product).astype(jnp.bfloat16)
    own_normed = lax.dynamic_slice_in_dim(tri_normed, quadrant_share * q_rows, q_rows, 0)
    closing = jax.nn.sigmoid(apply_linear(own_normed, trio_sigmoid_matrix)).reshape(
        q_rows, c_block, -1
    )
    change = apply_linear(product_normed, trio_final_matrix).reshape(q_rows, c_block, -1)
    out_rows = (mid_rows.astype(jnp.float32) + closing * change).astype(jnp.bfloat16)
    pairwise_output = lax.all_gather(out_rows, "branch", axis=0, tiled=True)
    return (revised_homolog_matrix, pairwise_output)


F32 = jnp.float32
BF16 = jnp.bfloat16
AXES = ("branch", "row", "col")
LANES = 128
HALF = LANES // 2
QUART = LANES // 4
PAD = 8


def lane_of(shape):
    return lax.broadcasted_iota(jnp.int32, shape, len(shape) - 1)


def roll(x, shift):
    shift %= x.shape[-1]
    return pltpu.roll(x, shift, x.ndim - 1) if shift else x


def dot_nn(a, b):
    return jnp.dot(a, b, preferred_element_type=F32)


def dot_nt(a, b):
    return lax.dot_general(a, b, (((1,), (1,)), ((), ())), preferred_element_type=F32)


def call(body, outs, scratch=(), flops=10**6, mib=8, sems=0, anywhere=0, out_hbm=0, alias=None):
    scratch = [pltpu.VMEM(s, d) for s, d in scratch]
    scratch += [pltpu.SemaphoreType.DMA] * sems
    far, near = pl.BlockSpec(memory_space=pltpu.HBM), pl.BlockSpec(memory_space=pltpu.VMEM)

    def run(*args):
        specs = {}
        if anywhere:
            specs["in_specs"] = [far] * anywhere + [near] * (len(args) - anywhere)
        if out_hbm:
            specs["out_specs"] = (far,) * out_hbm
        args = [
            pltpu.with_memory_space_constraint(x, pltpu.HBM) if n < anywhere else x
            for n, x in enumerate(args)
        ]
        return pl.pallas_call(
            body,
            out_shape=tuple(jax.ShapeDtypeStruct(s, d) for s, d in outs),
            scratch_shapes=scratch,
            compiler_params=pltpu.CompilerParams(vmem_limit_bytes=mib * 2**20),
            cost_estimate=pl.CostEstimate(flops=flops, bytes_accessed=2**19, transcendentals=0),
            input_output_aliases=alias or {},
            **specs,
        )(*args)

    return run


def project_body(
    rows, hom_h, left_h, right_h, couple_h, outer_h, offset_h, first_h, second_h,
    normed, left_t, right_t, couple, outer_w, offset, gates_w, scr, hom, left_w, right_w, *sems,
):
    parts = 2
    cut = hom.shape[0] // parts
    pieces = [pl.ds(n * cut, cut) for n in range(parts)]
    pairs = [(hom_h.at[p], hom.at[p]) for p in pieces]
    pairs += [(left_h, left_w), (right_h, right_w), (couple_h, couple), (outer_h, outer_w)]
    pairs += [(offset_h, offset), (first_h, gates_w.at[pl.ds(0, 2)])]
    pairs += [(second_h, gates_w.at[pl.ds(2, 2)])]
    moves = [pltpu.make_async_copy(src, dst, sem) for (src, dst), sem in zip(pairs, sems)]
    for move in moves[: parts + 2]:
        move.start()
    n_rows, depth = hom.shape
    share = n_rows // rows
    width = left_w.shape[0]
    step = 2
    for first in range(0, share, step):
        if first * rows % cut == 0:
            moves[first * rows // cut].wait()
        if first == 0:
            for move in moves[parts + 2 :]:
                move.start()
        x = hom[first * rows : (first + step) * rows, :].astype(F32)
        x = x - jnp.mean(x, axis=-1, keepdims=True)
        x = x * lax.rsqrt(jnp.mean(x * x, axis=-1, keepdims=True) + EPS)
        normed[first * rows : (first + step) * rows, :] = x.astype(BF16)
        for s in range(step):
            piece = x[s * rows : (s + 1) * rows, :]
            for part in range(depth // LANES):
                scr[part, pl.ds(first + s, rows, stride=share + PAD), :] = piece[
                    :, part * LANES : (part + 1) * LANES
                ]
    moves[parts].wait()
    moves[parts + 1].wait()
    weights = jnp.concatenate([left_w[...], right_w[...]], axis=0)
    acc = 0
    for part in range(depth // LANES):
        x = [scr[part, i * (share + PAD) : i * (share + PAD) + share, :] for i in range(rows)]
        x = jnp.concatenate(x, axis=0).astype(BF16)
        acc = acc + dot_nt(weights[:, part * LANES : (part + 1) * LANES], x)
    for g in range(n_rows // LANES):
        cut = slice(g * LANES, (g + 1) * LANES)
        left_t[g * width : (g + 1) * width, :] = acc[:width, cut].astype(BF16)
        right_t[g * width : (g + 1) * width, :] = acc[width:, cut].astype(BF16)
    for move in moves[parts + 2 :]:
        move.wait()


def heads_body(normed, key_w, value_w, query_w, gate_w, kv, query, gate):
    half = normed.shape[0] // 2
    x = normed[...]
    low = lane_of((half, LANES)) < HALF

    def both(w0, w1):
        y = dot_nt(x, jnp.concatenate([w0[...], w1[...]], axis=0))
        top, bottom = y[:half], y[half:]
        return (
            jnp.where(low, top, roll(bottom, HALF)),
            jnp.where(low, roll(top, HALF), bottom),
        )

    k, v = both(key_w, value_w)
    kv[:half, :] = k.astype(BF16)
    kv[half:, :] = v.astype(BF16)
    q, g = both(query_w, gate_w)
    query[...] = q.astype(BF16)
    gate[...] = jax.nn.sigmoid(g)


def pair_body(width, couple, offset_t, outer_w, left_t, couple_t, message, outer_wt, scr, wscr):
    tiles = couple.shape[0] // LANES
    for t in range(tiles):
        x = jnp.transpose(couple[t * LANES : (t + 1) * LANES, :])
        couple_t[t] = x
        x = x.astype(F32)
        x = x - jnp.mean(x, axis=0, keepdims=True)
        x = x * lax.rsqrt(jnp.mean(x * x, axis=0, keepdims=True) + EPS)
        scr[pl.ds(t, offset_t.shape[0], stride=tiles), :] = dot_nn(offset_t[...], x.astype(BF16))
    span = left_t.shape[0]
    message[:span, :] = left_t[...]
    message[span:, :] = scr[...].astype(BF16)
    per = LANES // width
    for p in range(width):
        cut = slice(p * width, (p + 1) * width)
        wscr[p * (width + PAD) : p * (width + PAD) + width, :] = outer_w[cut, :].astype(F32)
    for g in range(width // per):
        block = jnp.concatenate(
            [wscr[pl.ds(g * per + q, width, stride=width + PAD), :] for q in range(per)], axis=0
        )
        outer_wt[:, g * LANES : (g + 1) * LANES] = jnp.transpose(block.astype(BF16))


def gate_tiles(scr, norm_t, w_own, w_far, first):
    tiles = norm_t.shape[0]
    weights = jnp.concatenate(
        [w_own[first], w_far[first], w_own[first + 1], w_far[first + 1]], axis=0
    )
    half = weights.shape[0] // 2
    for t in range(0, tiles, 2):
        y = dot_nn(weights, jnp.concatenate([norm_t[t], norm_t[t + 1]], axis=1))
        gated = jax.nn.sigmoid(y[half:]) * y[:half]
        store_gated(scr, t, 2 * tiles + PAD, gated[:, :LANES])
        store_gated(scr, t + 1, 2 * tiles + PAD, gated[:, LANES:])


def drop_pad(scr, out, rows):
    for n in range(out.shape[0] // rows):
        at = n * (rows + PAD)
        out[n * rows : (n + 1) * rows, :] = scr[at : at + rows, :].astype(out.dtype)


def store_gated(scr, t, rows, gated):
    chans = gated.shape[0] // 2
    low = lane_of((chans, LANES)) < HALF
    a, b = gated[:chans], gated[chans:]
    scr[pl.ds(2 * t, chans, stride=rows), :] = jnp.where(low, a, roll(b, HALF))
    scr[pl.ds(2 * t + 1, chans, stride=rows), :] = jnp.where(low, roll(a, HALF), b)


def outer_body(
    total_rows, couple_t, outer_wt, left_own, left_far, own_r, sib_r, got, got_sib,
    mid_t, norm_t, lhs, rscr, mscr,
):
    col = lax.axis_index("col")
    row = lax.axis_index("row")
    chip_y, core = row // 2, row % 2
    width = lhs.shape[0] // couple_t.shape[0]
    span = own_r.shape[0] // width * LANES
    tiles = couple_t.shape[0]
    rows = 2 * tiles
    share = span // rows
    block = rows * 2
    group = lane_of((width, LANES)) // share
    own_first = col == 0
    for g in range(span // LANES):
        cut = slice(g * width, (g + 1) * width)
        own, far = left_own[cut, :].astype(F32), left_far[cut, :].astype(F32)
        a, b = jnp.where(own_first, own, far), jnp.where(own_first, far, own)
        even = jnp.where(
            group == 0, a,
            jnp.where(group == 1, roll(b, QUART), jnp.where(group == 2, roll(a, QUART), roll(b, HALF))),
        )
        odd = jnp.where(
            group == 0, roll(a, HALF),
            jnp.where(group == 1, roll(b, -QUART), jnp.where(group == 2, roll(a, -QUART), b)),
        )
        lhs[2 * g * width : (2 * g + 1) * width, :] = even.astype(BF16)
        lhs[(2 * g + 1) * width : (2 * g + 2) * width, :] = odd.astype(BF16)
    here, north = chip_y == col, core == 0
    size = own_r.shape[0]
    for a in range(2):
        for g in range(span // LANES):
            cut = slice(g * width, (g + 1) * width)
            same = slice(a * size + g * width, a * size + (g + 1) * width)
            flip = slice((1 - a) * size + g * width, (1 - a) * size + (g + 1) * width)
            from_0 = jnp.where(north, got[same, :], got_sib[same, :])
            from_1 = jnp.where(north, got_sib[flip, :], got[flip, :])
            local = jnp.where(core == a, own_r[cut, :], sib_r[cut, :])
            one = jnp.where(here, local, from_0).astype(F32)
            two = jnp.where(here, from_0, from_1).astype(F32)
            t0, t1 = jnp.where(own_first, one, two), jnp.where(own_first, two, one)
            for j4 in range(LANES // share):
                j = a * rows + g * (LANES // share) + j4
                tile = jnp.where(
                    group == 0, roll(t0, -share * j4),
                    jnp.where(group == 1, roll(t1, share - share * j4), 0.0),
                )
                rscr[pl.ds(j, width, stride=2 * block + PAD), :] = tile
                rscr[pl.ds(block + j, width, stride=2 * block + PAD), :] = roll(tile, HALF)
    left = lhs[...]
    for q in range(0, width, 2):
        at = [n * (LANES + PAD) for n in (q, q + 1)]
        rhs = jnp.concatenate([rscr[n : n + LANES, :] for n in at], axis=0).astype(BF16)
        prod = dot_nt(left, rhs).astype(BF16)
        for t in range(tiles):
            for e in range(2):
                mscr[t, (q + e) * width : (q + e + 1) * width, :] = prod[
                    t * width : (t + 1) * width, e * LANES : (e + 1) * LANES
                ]
    for t in range(0, tiles, 2):
        both = dot_nn(outer_wt[...], jnp.concatenate([mscr[t], mscr[t + 1]], axis=1))
        for e in range(2):
            update = both[:, e * LANES : (e + 1) * LANES] * (1.0 / total_rows)
            mid = (couple_t[t + e].astype(F32) + update).astype(BF16)
            mid_t[t + e] = mid
            x = mid.astype(F32)
            x = x - jnp.mean(x, axis=0, keepdims=True)
            x = x * lax.rsqrt(jnp.mean(x * x, axis=0, keepdims=True) + EPS)
            norm_t[t + e] = x.astype(BF16)


def right_body(norm_t, w_own, w_far, right_pk, gscr):
    gate_tiles(gscr, norm_t, w_own, w_far, 2)
    drop_pad(gscr, right_pk, 2 * norm_t.shape[0])


def left_body(norm_t, w_own, w_far, left_pk, gscr):
    gate_tiles(gscr, norm_t, w_own, w_far, 0)
    drop_pad(gscr, left_pk, 2 * norm_t.shape[0])


def close_body(norm_t, close_w, close_t):
    w_close = jnp.transpose(close_w[...].astype(F32)).astype(BF16)
    for t in range(norm_t.shape[0]):
        close_t[t] = jax.nn.sigmoid(dot_nn(w_close, norm_t[t]))


def triangle_body(rows, part, left_pk, own, sib, across, across_sib, mine, other):
    col = lax.axis_index("col")
    row = lax.axis_index("row")
    chip_y, core = row // 2, row % 2
    is_low, here = core == 0, chip_y == col
    n = rows // 2
    low = lane_of((n, LANES)) < HALF
    for ch in range(left_pk.shape[0] // rows):
        cut = slice(ch * rows, (ch + 1) * rows)
        a = left_pk[ch * rows + part * n : ch * rows + (part + 1) * n, :]
        zero = jnp.zeros_like(a)
        lhs = jnp.concatenate([jnp.where(low, a, zero), jnp.where(low, zero, a)], axis=0)
        o, s, x, xs = own[cut, :], sib[cut, :], across[cut, :], across_sib[cut, :]
        n0, n1 = jnp.where(is_low, o, s), jnp.where(is_low, s, o)
        f0, f1 = jnp.where(is_low, x, xs), jnp.where(is_low, xs, x)
        rhs = jnp.concatenate(
            [
                jnp.where(here, n0, f0), jnp.where(here, n1, f1),
                jnp.where(here, f0, n0), jnp.where(here, f1, n1),
            ],
            axis=0,
        )
        prod = dot_nt(lhs, rhs)
        u, v = prod[:n], prod[n:]
        to = slice(ch * n, (ch + 1) * n)
        mine[to, :] = jnp.where(low, u, roll(v, HALF))
        other[to, :] = jnp.where(low, roll(u, HALF), v).astype(BF16)


def final_body(n, part, *refs):
    half_own, half_far, mid_t, close_t, final_w, out_h, scr, out, *sems = refs[part:]
    branch = lax.axis_index("branch")
    chans = half_own.shape[0] // n
    low = lane_of((chans, LANES)) < HALF
    for h, half in enumerate((half_own, half_far)):
        for c in range(chans):
            scr[h, c * (n + PAD) : c * (n + PAD) + n, :] = half[c * n : (c + 1) * n, :].astype(F32)
    owners = [branch, branch ^ 2, branch ^ 1, branch ^ 3]
    w_t = [final_w[pl.ds(pl.multiple_of(o * chans, chans), chans), :] for o in owners]
    w_t = jnp.transpose(jnp.concatenate(w_t, axis=0).astype(F32)).astype(BF16)
    tiles = n // 2
    per = tiles // len(sems)
    base = part * tiles
    moves = []

    def normed(t):
        blocks = []
        for h in range(2):
            z0 = scr[h, pl.ds(2 * t, chans, stride=n + PAD), :]
            z1 = scr[h, pl.ds(2 * t + 1, chans, stride=n + PAD), :]
            blocks += [jnp.where(low, z0, roll(z1, HALF)), jnp.where(low, roll(z0, HALF), z1)]
        x = jnp.concatenate(blocks, axis=0)
        x = x - jnp.mean(x, axis=0, keepdims=True)
        x = x * lax.rsqrt(jnp.mean(x * x, axis=0, keepdims=True) + EPS)
        return x.astype(BF16)

    for start in range(0, tiles, per):
        change = dot_nn(
            w_t, jnp.concatenate([normed(t) for t in range(start, start + per)], axis=1)
        )
        for e in range(per):
            t = start + e
            part_of = change[:, e * LANES : (e + 1) * LANES]
            result = mid_t[base + t].astype(F32) + close_t[base + t] * part_of
            out[t * LANES : (t + 1) * LANES, :] = jnp.transpose(result.astype(BF16))
        here = out.at[pl.ds(start * LANES, per * LANES)]
        there = out_h.at[pl.ds((base + start) * LANES, per * LANES)]
        moves.append(pltpu.make_async_copy(here, there, sems[start // per]))
        moves[-1].start()
    for move in moves:
        move.wait()


def attend_body(
    rows, head, query, gate, own, sib, across, across_sib, sent, got, w_out, *rest
):
    outs, (bscr, cscr) = rest[:-2], rest[-2:]
    col = lax.axis_index("col")
    row = lax.axis_index("row")
    branch = lax.axis_index("branch")
    top, is_low = row // 2 == 0, row % 2 == 0
    half = query.shape[0]
    scale = float(head) ** (-0.5)
    n_bias = bscr.shape[0] // 2
    start = sent.shape[0] - n_bias
    b_own, b_far = sent[start:, :].astype(F32), got[start:, :].astype(F32)
    b0, b1 = jnp.where(col == 0, b_own, b_far), jnp.where(col == 0, b_far, b_own)
    low = lane_of((n_bias, LANES)) < HALF
    bscr[pl.ds(0, n_bias, stride=2), :] = jnp.where(low, b0, roll(b1, HALF))
    bscr[pl.ds(1, n_bias, stride=2), :] = jnp.where(low, roll(b0, HALF), b1)
    bias = jnp.transpose(jnp.concatenate([bscr[...], bscr[...]], axis=0))
    b = [bias[n * rows : (n + 1) * rows] for n in range(LANES // rows)]
    b = [jnp.where(is_low, b[n], b[n ^ 1]) for n in range(len(b))]
    b = [jnp.where(top, b[n], b[n ^ 2]) for n in range(len(b))]
    bias = jnp.concatenate(b, axis=0)
    group = lane_of((rows, LANES)) // head

    def gather(at):
        cut = pl.ds(pl.multiple_of(at, rows), rows)
        return jnp.concatenate([own[cut, :], sib[cut, :], across[cut, :], across_sib[cut, :]], axis=0)

    batch = 4

    def some(step, carry):
        spots = [(step * batch + n) * rows for n in range(batch)]
        cuts = [pl.ds(pl.multiple_of(at, rows), rows) for at in spots]
        masked = []
        for cut in cuts:
            q = query[cut, :]
            zero = jnp.zeros_like(q)
            masked.append(
                jnp.concatenate(
                    [jnp.where(group == g, q, zero) for g in range(LANES // head)], axis=0
                )
            )
        scores = [dot_nt(gather(at), q) * scale + bias for at, q in zip(spots, masked)]
        tops = [jnp.max(x, axis=0, keepdims=True) for x in scores]
        expo = [jnp.exp(x - top) for x, top in zip(scores, tops)]
        expo = [x * (1.0 / jnp.sum(x, axis=0, keepdims=True)) for x in expo]
        full = [
            lax.dot_general(
                x.astype(BF16), gather(half + at), (((0,), (0,)), ((), ())),
                preferred_element_type=F32,
            )
            for x, at in zip(expo, spots)
        ]
        for cut, x in zip(cuts, full):
            ctx = x[:rows]
            for g in range(1, LANES // head):
                ctx = jnp.where(group == g, x[g * rows : (g + 1) * rows], ctx)
            cscr[cut, :] = (ctx * gate[cut, :]).astype(BF16)
        return carry

    lax.fori_loop(0, half // rows // batch, some, 0, unroll=True)
    ctx = cscr[...]
    low = lane_of((w_out.shape[0], LANES)) < HALF
    for m in range(len(outs)):
        chunk = branch ^ m
        at = pl.multiple_of((chunk // 2) * LANES, LANES)
        w = w_out[:, pl.ds(at, LANES)].astype(F32)
        w = jnp.where(chunk % 2 == 0, w, roll(w, HALF))
        w = jnp.concatenate([jnp.where(low, w, 0.0), jnp.where(low, 0.0, roll(w, HALF))], axis=0)
        outs[m][...] = dot_nn(ctx, w.astype(BF16)).astype(BF16)


def revise_body(hom, p0, p1, p2, p3, out):
    branch = lax.axis_index("branch")
    acc = p0[...].astype(F32) + p1[...].astype(F32)
    acc = acc + p2[...].astype(F32) + p3[...].astype(F32)
    n = acc.shape[0]
    at = pl.multiple_of((branch // 2) * LANES, LANES)
    base = hom[:, pl.ds(at, LANES)].astype(F32)
    base = jnp.where(branch % 2 == 0, base, roll(base, HALF))
    out[:n, :] = (acc + base[:n])[:, :HALF].astype(BF16)
    out[n:, :] = (roll(acc, HALF) + base[n:])[:, :HALF].astype(BF16)


def fast_per_device(
    mesh,
    homolog_tensor,
    couple_tensor,
    probe_matrix,
    lookup_matrix,
    content_matrix,
    scoring_sigmoid_matrix,
    scoring_final_matrix,
    couple_offset_matrix,
    product_first_matrix,
    product_second_matrix,
    product_final_matrix,
    trio_first_matrix,
    trio_second_matrix,
    trio_sigmoid_matrix,
    trio_final_matrix,
):
    n_b, n_r, n_c = (mesh.shape[a] for a in AXES)

    def send(x, source):
        pairs = []
        for b in range(n_b):
            for r in range(n_r):
                for c in range(n_c):
                    if (origin := source(b, r, c)) is not None:
                        sb, sr, sc = origin
                        pairs.append(((sb * n_r + sr) * n_c + sc, (b * n_r + r) * n_c + c))
        return lax.ppermute(x, AXES, pairs)

    def other_col(b, r, c):
        return b, r, c ^ 1

    def other_core(b, r, c):
        return b, r ^ 1, c

    def other_chip(b, r, c):
        return b, r ^ 2, c

    def turned(b, r, c):
        y, core = r // 2, r % 2
        if y == c:
            return None if core else (b, r, c ^ 1)
        return b, 2 * c + core, c ^ core

    share, rows, depth = homolog_tensor.shape
    block = couple_tensor.shape[1]
    chans = couple_tensor.shape[2]
    width = product_first_matrix.shape[1]
    heads_w = probe_matrix.shape[1]
    local_heads = couple_offset_matrix.shape[1]
    head = heads_w // local_heads
    quarter = trio_first_matrix.shape[2]
    tiles = rows * block // LANES
    n_rows = share * rows
    hom = homolog_tensor.reshape(n_rows, depth)
    couple = couple_tensor.reshape(rows * block, chans)

    flat = (n_rows * width // LANES, LANES)
    normed, left_t, right_t, couple_v, outer_w, offset_t, w_own = call(
        functools.partial(project_body, rows),
        [
            ((n_rows, depth), BF16), (flat, BF16), (flat, BF16),
            (couple.shape, BF16), (product_final_matrix.shape, BF16),
            ((local_heads, chans), BF16), ((4, quarter, chans), BF16),
        ],
        [
            ((depth // LANES, rows * (share + PAD), LANES), F32), ((n_rows, depth), BF16),
            ((width, depth), BF16), ((width, depth), BF16),
        ],
        sems=9,
        anywhere=8,
    )(
        hom, product_first_matrix.T, product_second_matrix.T, couple, product_final_matrix,
        couple_offset_matrix.T, jnp.transpose(trio_first_matrix, (0, 2, 1)),
        jnp.transpose(trio_second_matrix, (0, 2, 1)),
    )
    sib_r = send(right_t, other_core)
    got_r = send(jnp.concatenate([right_t, sib_r], axis=0), turned)
    couple_t, message, outer_wt = call(
        functools.partial(pair_body, width),
        [
            ((tiles, chans, LANES), BF16),
            ((flat[0] + local_heads * tiles, LANES), BF16),
            ((chans, width * width), BF16),
        ],
        [((local_heads * tiles, LANES), F32), ((width * (width + PAD), chans), F32)],
    )(couple_v, offset_t, outer_w, left_t)
    got = send(message, other_col)
    kv, query, gate = call(
        heads_body,
        [((n_rows, LANES), BF16), ((n_rows // 2, LANES), BF16), ((n_rows // 2, LANES), F32)],
    )(normed, lookup_matrix.T, content_matrix.T, probe_matrix.T, scoring_sigmoid_matrix.T)
    kv_x = send(kv, other_chip)
    kv_s = send(kv, other_core)
    kv_xs = send(kv_x, other_core)
    w_far = send(w_own, lambda b, r, c: (b ^ 2, r, c))
    got_rs = send(got_r, other_core)

    mid_t, norm_t = call(
        functools.partial(outer_body, share * n_c),
        [((tiles, chans, LANES), BF16), ((tiles, chans, LANES), BF16)],
        [
            ((tiles * width, LANES), BF16),
            ((width * (LANES + PAD), LANES), F32),
            ((tiles, width * width, LANES), BF16),
        ],
        mib=16,
    )(couple_t, outer_wt, message, got, right_t, sib_r, got_r, got_rs)
    (right_pk,) = call(
        right_body, [((quarter * rows, LANES), BF16)], [((quarter * (rows + PAD), LANES), F32)]
    )(norm_t, w_own, w_far)
    right_x = send(right_pk, other_chip)
    right_s = send(right_pk, other_core)
    (left_pk,) = call(
        left_body, [((quarter * rows, LANES), BF16)], [((quarter * (rows + PAD), LANES), F32)]
    )(norm_t, w_own, w_far)
    parts = call(
        functools.partial(attend_body, rows, head),
        [((n_rows // 2, LANES), BF16)] * n_b,
        [((local_heads * rows, LANES), F32), ((n_rows // 2, LANES), BF16)],
    )(query, gate, kv, kv_s, kv_x, kv_xs, message, got, scoring_final_matrix)
    right_xs = send(right_x, other_core)

    mines, fars = [], []
    for part in range(2):
        mine, other = call(
            functools.partial(triangle_body, rows, part),
            [((quarter * rows // 2, LANES), F32), ((quarter * rows // 2, LANES), BF16)],
        )(left_pk, right_pk, right_s, right_x, right_xs)
        mines.append(mine)
        fars.append(send(other, other_col))
    (close_t,) = call(close_body, [((tiles, chans, LANES), F32)])(norm_t, trio_sigmoid_matrix)
    parts = [parts[0]] + [send(parts[m], lambda b, r, c, m=m: (b ^ m, r, c)) for m in range(1, n_b)]
    half_own = [(mine + far.astype(F32)).astype(BF16) for mine, far in zip(mines, fars)]
    half_far = [send(half, lambda b, r, c: (b ^ 1, r, c)) for half in half_own]
    (revised,) = call(revise_body, [((n_rows, depth // n_b), BF16)])(hom, *parts)

    pair_out = ()
    for part in range(2):
        pair_out = call(
            functools.partial(final_body, rows // 2, part),
            [((rows * block, chans), BF16)],
            [((2, quarter * (rows // 2 + PAD), LANES), F32), ((rows * block // 2, chans), BF16)],
            mib=12,
            sems=4,
            out_hbm=1,
            anywhere=part,
            alias={0: 0} if part else None,
        )(*pair_out, half_own[part], half_far[part], mid_t, close_t, trio_final_matrix)
    (pair_out,) = pair_out
    return (
        revised.reshape(share, rows, depth // n_b),
        pair_out.reshape(rows, block, chans),
    )


def fits(mesh, args):
    hom, couple = args[0], args[1]
    share, rows, depth = hom.shape
    return (
        mesh.shape["branch"] == 4
        and mesh.shape["row"] == 4
        and mesh.shape["col"] == 2
        and couple.shape[0] == rows
        and couple.shape[1] == 2 * rows == HALF
        and couple.shape[2] == LANES
        and share == QUART
        and args[2].shape[1] == HALF
        and depth == 4 * HALF
        and args[8].shape[1] == QUART
        and args[11].shape[2] == QUART
        and args[7].shape[1] == 2
    )


def dispatch(mesh, *args):
    if fits(mesh, args):
        return fast_per_device(mesh, *args)
    return plain_per_device(*args)


def solution(mesh):
    return jax.shard_map(
        functools.partial(dispatch, mesh),
        mesh=mesh,
        in_specs=(
            P("col", "row", None),
            P("row", "col", None),
            P(None, "branch"),
            P(None, "branch"),
            P(None, "branch"),
            P(None, "branch"),
            P("branch", None),
            P(None, "branch"),
            P(),
            P(),
            P(),
            P(None, None, "branch"),
            P(None, None, "branch"),
            P(),
            P(),
        ),
        out_specs=(P("col", "row", "branch"), P("row", "col", None)),
        check_vma=False,
    )
```

```python
import functools

import jax
import jax.numpy as jnp
from jax import lax
from jax.experimental import pallas as pl
from jax.experimental.pallas import tpu as pltpu
from jax.sharding import PartitionSpec as P


EPS = 1e-05


def spread_2(block, axis, owner):
    block = jnp.where(lax.axis_index(axis) == owner, block, jnp.zeros_like(block))
    return lax.psum(block, axis)


def standardise_rows(values):
    values = values.astype(jnp.float32)
    centred = values - jnp.mean(values, axis=-1, keepdims=True)
    variance = jnp.mean(centred * centred, axis=-1, keepdims=True)
    return centred / jnp.sqrt(variance + EPS)


def apply_linear(source, weights):
    return jnp.dot(
        source.reshape(-1, weights.shape[0]), weights, preferred_element_type=jnp.float32
    )


def attend(query, key, value, bias):
    scale = float(query.shape[-1]) ** (-0.5)
    scores = jnp.einsum("sihd,sjhd->shij", query, key, preferred_element_type=jnp.float32) * scale
    scores = scores + jnp.transpose(bias, (2, 0, 1)).astype(jnp.float32)[None]
    top = jnp.max(scores, axis=-1, keepdims=True)
    expo = jnp.exp(scores - top)
    total = jnp.sum(expo, axis=-1)
    summed = jnp.einsum(
        "shij,sjhd->sihd", expo.astype(jnp.bfloat16), value, preferred_element_type=jnp.float32
    )
    return summed / jnp.transpose(total, (0, 2, 1))[..., None]


def plain_per_device(
    homolog_tensor,
    couple_tensor,
    probe_matrix,
    lookup_matrix,
    content_matrix,
    scoring_sigmoid_matrix,
    scoring_final_matrix,
    couple_offset_matrix,
    product_first_matrix,
    product_second_matrix,
    product_final_matrix,
    trio_first_matrix,
    trio_second_matrix,
    trio_sigmoid_matrix,
    trio_final_matrix,
):
    branches = lax.axis_size("branch")
    rows_count = lax.axis_size("row")
    cols_count = lax.axis_size("col")
    quadrant_share = lax.axis_index("branch")
    col_index = lax.axis_index("col")
    homolog_share, position_tile, channel_extent = homolog_tensor.shape
    c_block = couple_tensor.shape[1]
    residues = position_tile * rows_count
    depth = probe_matrix.shape[1]
    local_heads = couple_offset_matrix.shape[1]
    head_size = depth // local_heads
    q_rows = position_tile // branches
    total_rows = homolog_share * cols_count
    outer_width = product_first_matrix.shape[1]
    standardised_tensor = standardise_rows(homolog_tensor).astype(jnp.bfloat16)
    pair_normed = standardise_rows(couple_tensor).astype(jnp.bfloat16)
    bias_tile = (
        apply_linear(pair_normed, couple_offset_matrix)
        .astype(jnp.bfloat16)
        .reshape(position_tile, c_block, local_heads)
    )
    bias_band = lax.all_gather(bias_tile, "col", axis=1, tiled=True)
    spread = lax.all_to_all(standardised_tensor, "row", split_axis=0, concat_axis=1, tiled=True)
    few = spread.shape[0]
    shaped = (few, residues, local_heads, head_size)
    query = apply_linear(spread, probe_matrix).astype(jnp.bfloat16).reshape(shaped)
    key = apply_linear(spread, lookup_matrix).astype(jnp.bfloat16).reshape(shaped)
    value = apply_linear(spread, content_matrix).astype(jnp.bfloat16).reshape(shaped)
    gate_pre = apply_linear(spread, scoring_sigmoid_matrix).reshape(shaped)
    bias_full = lax.all_gather(bias_band, "row", axis=0, tiled=True)
    attended_values = attend(query, key, value, bias_full) * jax.nn.sigmoid(gate_pre)
    attended_values = attended_values.astype(jnp.bfloat16).reshape(few, residues, depth)
    attended_values = lax.all_to_all(
        attended_values, "row", split_axis=1, concat_axis=0, tiled=True
    )
    joined_tensor = apply_linear(attended_values, scoring_final_matrix).reshape(
        homolog_share, position_tile, channel_extent
    )
    joined_tensor = lax.psum_scatter(
        joined_tensor.astype(jnp.bfloat16), "branch", scatter_dimension=2, tiled=True
    ).astype(jnp.float32)
    device_share = channel_extent // branches
    local_alignment = lax.dynamic_slice_in_dim(
        homolog_tensor, quadrant_share * device_share, device_share, 2
    )
    revised_homolog_matrix = (local_alignment.astype(jnp.float32) + joined_tensor).astype(
        jnp.bfloat16
    )
    left_rows = lax.dynamic_slice_in_dim(standardised_tensor, quadrant_share * q_rows, q_rows, 1)
    left_outer = (
        apply_linear(left_rows, product_first_matrix)
        .astype(jnp.bfloat16)
        .reshape(homolog_share, q_rows * outer_width)
    )
    right_local = (
        apply_linear(standardised_tensor, product_second_matrix)
        .astype(jnp.bfloat16)
        .reshape(homolog_share, position_tile, outer_width)
    )
    right_outer = lax.all_gather(right_local, "row", axis=1, tiled=True)
    wide_out = product_final_matrix.astype(jnp.float32)
    left_major = jnp.transpose(left_outer)
    count = lax.axis_size("col") * c_block
    piece = right_outer.reshape(homolog_share, count * outer_width)
    outer = jnp.dot(left_major, piece, preferred_element_type=jnp.float32)
    outer = outer.reshape(q_rows, outer_width, count, outer_width)
    outer = jnp.transpose(outer, (2, 0, 1, 3)).reshape(count * q_rows, outer_width * outer_width)
    term = jnp.dot(outer, wide_out, precision=lax.Precision.HIGHEST) / total_rows
    update = lax.psum_scatter(
        term.reshape(count, q_rows, wide_out.shape[1]).astype(jnp.bfloat16),
        "col",
        scatter_dimension=0,
        tiled=True,
    ).astype(jnp.float32)
    update = jnp.transpose(update, (1, 0, 2))
    pair_rows = lax.dynamic_slice_in_dim(couple_tensor, quadrant_share * q_rows, q_rows, 0)
    mid_rows = (pair_rows.astype(jnp.float32) + update).astype(jnp.bfloat16)
    pair_mid = lax.all_gather(mid_rows, "branch", axis=0, tiled=True)
    tri_normed = standardise_rows(pair_mid).astype(jnp.bfloat16)

    def gated(weights):
        linear = apply_linear(tri_normed, weights[0])
        opening = apply_linear(tri_normed, weights[1])
        return (
            (jax.nn.sigmoid(opening) * linear)
            .astype(jnp.bfloat16)
            .reshape(position_tile, c_block, weights.shape[2])
        )

    tri_left = gated(trio_first_matrix)
    tri_right = gated(trio_second_matrix)
    left_band, right_band = (
        lax.all_gather(tri_left, "col", axis=1, tiled=True),
        lax.all_gather(tri_right, "col", axis=1, tiled=True),
    )
    ratio = rows_count // cols_count

    def mirror(offset):
        return spread_2(right_band, "row", col_index * ratio + offset)

    right_cols = jnp.concatenate([mirror(offset) for offset in range(ratio)], axis=0)
    product = jnp.einsum("ikc,jkc->ijc", left_band, right_cols, preferred_element_type=jnp.float32)
    product = lax.all_to_all(product, "branch", split_axis=0, concat_axis=2, tiled=True)
    product_normed = standardise_rows(product).astype(jnp.bfloat16)
    own_normed = lax.dynamic_slice_in_dim(tri_normed, quadrant_share * q_rows, q_rows, 0)
    closing = jax.nn.sigmoid(apply_linear(own_normed, trio_sigmoid_matrix)).reshape(
        q_rows, c_block, -1
    )
    change = apply_linear(product_normed, trio_final_matrix).reshape(q_rows, c_block, -1)
    out_rows = (mid_rows.astype(jnp.float32) + closing * change).astype(jnp.bfloat16)
    pairwise_output = lax.all_gather(out_rows, "branch", axis=0, tiled=True)
    return (revised_homolog_matrix, pairwise_output)


F32 = jnp.float32
BF16 = jnp.bfloat16
AXES = ("branch", "row", "col")
LANES = 128
HALF = LANES // 2
QUART = LANES // 4
PAD = 8


def lane_of(shape):
    return lax.broadcasted_iota(jnp.int32, shape, len(shape) - 1)


def roll(x, shift):
    shift %= x.shape[-1]
    return pltpu.roll(x, shift, x.ndim - 1) if shift else x


def dot_nn(a, b):
    return jnp.dot(a, b, preferred_element_type=F32)


def dot_nt(a, b):
    return lax.dot_general(a, b, (((1,), (1,)), ((), ())), preferred_element_type=F32)


def call(body, outs, scratch=(), flops=10**6, mib=8, sems=0, anywhere=0, out_hbm=0, alias=None):
    scratch = [pltpu.VMEM(s, d) for s, d in scratch]
    scratch += [pltpu.SemaphoreType.DMA] * sems
    far, near = pl.BlockSpec(memory_space=pltpu.HBM), pl.BlockSpec(memory_space=pltpu.VMEM)

    def run(*args):
        specs = {}
        if anywhere:
            specs["in_specs"] = [far] * anywhere + [near] * (len(args) - anywhere)
        if out_hbm:
            specs["out_specs"] = (far,) * out_hbm
        args = [
            pltpu.with_memory_space_constraint(x, pltpu.HBM) if n < anywhere else x
            for n, x in enumerate(args)
        ]
        return pl.pallas_call(
            body,
            out_shape=tuple(jax.ShapeDtypeStruct(s, d) for s, d in outs),
            scratch_shapes=scratch,
            compiler_params=pltpu.CompilerParams(vmem_limit_bytes=mib * 2**20),
            cost_estimate=pl.CostEstimate(flops=flops, bytes_accessed=2**19, transcendentals=0),
            input_output_aliases=alias or {},
            **specs,
        )(*args)

    return run


def project_body(
    rows, hom_h, left_h, right_h, couple_h, outer_h, offset_h, first_h, second_h,
    normed, left_t, right_t, couple, outer_w, offset, gates_w, scr, hom, left_w, right_w, *sems,
):
    parts = 2
    cut = hom.shape[0] // parts
    pieces = [pl.ds(n * cut, cut) for n in range(parts)]
    pairs = [(hom_h.at[p], hom.at[p]) for p in pieces]
    pairs += [(left_h, left_w), (right_h, right_w), (couple_h, couple), (outer_h, outer_w)]
    pairs += [(offset_h, offset), (first_h, gates_w.at[pl.ds(0, 2)])]
    pairs += [(second_h, gates_w.at[pl.ds(2, 2)])]
    moves = [pltpu.make_async_copy(src, dst, sem) for (src, dst), sem in zip(pairs, sems)]
    for move in moves[: parts + 2]:
        move.start()
    n_rows, depth = hom.shape
    share = n_rows // rows
    width = left_w.shape[0]
    step = 2
    for first in range(0, share, step):
        if first * rows % cut == 0:
            moves[first * rows // cut].wait()
        if first == 0:
            for move in moves[parts + 2 :]:
                move.start()
        x = hom[first * rows : (first + step) * rows, :].astype(F32)
        x = x - jnp.mean(x, axis=-1, keepdims=True)
        x = x * lax.rsqrt(jnp.mean(x * x, axis=-1, keepdims=True) + EPS)
        normed[first * rows : (first + step) * rows, :] = x.astype(BF16)
        for s in range(step):
            piece = x[s * rows : (s + 1) * rows, :]
            for part in range(depth // LANES):
                scr[part, pl.ds(first + s, rows, stride=share + PAD), :] = piece[
                    :, part * LANES : (part + 1) * LANES
                ]
    moves[parts].wait()
    moves[parts + 1].wait()
    weights = jnp.concatenate([left_w[...], right_w[...]], axis=0)
    acc = 0
    for part in range(depth // LANES):
        x = [scr[part, i * (share + PAD) : i * (share + PAD) + share, :] for i in range(rows)]
        x = jnp.concatenate(x, axis=0).astype(BF16)
        acc = acc + dot_nt(weights[:, part * LANES : (part + 1) * LANES], x)
    for g in range(n_rows // LANES):
        cut = slice(g * LANES, (g + 1) * LANES)
        left_t[g * width : (g + 1) * width, :] = acc[:width, cut].astype(BF16)
        right_t[g * width : (g + 1) * width, :] = acc[width:, cut].astype(BF16)
    for move in moves[parts + 2 :]:
        move.wait()


def heads_body(normed, key_w, value_w, query_w, gate_w, kv, query, gate):
    half = normed.shape[0] // 2
    x = normed[...]
    low = lane_of((half, LANES)) < HALF

    weights = [w[...] for w in (key_w, value_w, query_w, gate_w)]
    full = dot_nt(x, jnp.concatenate(weights, axis=0))

    def both(y):
        top, bottom = y[:half], y[half:]
        return (
            jnp.where(low, top, roll(bottom, HALF)),
            jnp.where(low, roll(top, HALF), bottom),
        )

    k, v = both(full[:, :LANES])
    kv[:half, :] = k.astype(BF16)
    kv[half:, :] = v.astype(BF16)
    q, g = both(full[:, LANES:])
    query[...] = q.astype(BF16)
    gate[...] = jax.nn.sigmoid(g)


def pair_body(width, couple, offset_t, outer_w, left_t, couple_t, message, outer_wt, scr, wscr):
    tiles = couple.shape[0] // LANES
    for t in range(tiles):
        x = jnp.transpose(couple[t * LANES : (t + 1) * LANES, :])
        couple_t[t] = x
        x = x.astype(F32)
        x = x - jnp.mean(x, axis=0, keepdims=True)
        x = x * lax.rsqrt(jnp.mean(x * x, axis=0, keepdims=True) + EPS)
        scr[pl.ds(t, offset_t.shape[0], stride=tiles), :] = dot_nn(offset_t[...], x.astype(BF16))
    span = left_t.shape[0]
    message[:span, :] = left_t[...]
    message[span:, :] = scr[...].astype(BF16)
    per = LANES // width
    for p in range(width):
        cut = slice(p * width, (p + 1) * width)
        wscr[p * (width + PAD) : p * (width + PAD) + width, :] = outer_w[cut, :].astype(F32)
    for g in range(width // per):
        block = jnp.concatenate(
            [wscr[pl.ds(g * per + q, width, stride=width + PAD), :] for q in range(per)], axis=0
        )
        outer_wt[:, g * LANES : (g + 1) * LANES] = jnp.transpose(block.astype(BF16))


def gate_tiles(scr, norm_t, w_own, w_far, first):
    tiles = norm_t.shape[0]
    weights = jnp.concatenate(
        [w_own[first], w_far[first], w_own[first + 1], w_far[first + 1]], axis=0
    )
    half = weights.shape[0] // 2
    for t in range(0, tiles, 2):
        y = dot_nn(weights, jnp.concatenate([norm_t[t], norm_t[t + 1]], axis=1))
        gated = jax.nn.sigmoid(y[half:]) * y[:half]
        store_gated(scr, t, 2 * tiles + PAD, gated[:, :LANES])
        store_gated(scr, t + 1, 2 * tiles + PAD, gated[:, LANES:])


def drop_pad(scr, out, rows):
    for n in range(out.shape[0] // rows):
        at = n * (rows + PAD)
        out[n * rows : (n + 1) * rows, :] = scr[at : at + rows, :].astype(out.dtype)


def store_gated(scr, t, rows, gated):
    chans = gated.shape[0] // 2
    low = lane_of((chans, LANES)) < HALF
    a, b = gated[:chans], gated[chans:]
    scr[pl.ds(2 * t, chans, stride=rows), :] = jnp.where(low, a, roll(b, HALF))
    scr[pl.ds(2 * t + 1, chans, stride=rows), :] = jnp.where(low, roll(a, HALF), b)


def outer_body(
    total_rows, couple_t, outer_wt, left_own, left_far, own_r, sib_r, got, got_sib,
    mid_t, norm_t, lhs, rscr, mscr,
):
    col = lax.axis_index("col")
    row = lax.axis_index("row")
    chip_y, core = row // 2, row % 2
    width = lhs.shape[0] // couple_t.shape[0]
    span = own_r.shape[0] // width * LANES
    tiles = couple_t.shape[0]
    rows = 2 * tiles
    share = span // rows
    block = rows * 2
    group = lane_of((width, LANES)) // share
    own_first = col == 0
    for g in range(span // LANES):
        cut = slice(g * width, (g + 1) * width)
        own, far = left_own[cut, :].astype(F32), left_far[cut, :].astype(F32)
        a, b = jnp.where(own_first, own, far), jnp.where(own_first, far, own)
        even = jnp.where(
            group == 0, a,
            jnp.where(group == 1, roll(b, QUART), jnp.where(group == 2, roll(a, QUART), roll(b, HALF))),
        )
        odd = jnp.where(
            group == 0, roll(a, HALF),
            jnp.where(group == 1, roll(b, -QUART), jnp.where(group == 2, roll(a, -QUART), b)),
        )
        lhs[2 * g * width : (2 * g + 1) * width, :] = even.astype(BF16)
        lhs[(2 * g + 1) * width : (2 * g + 2) * width, :] = odd.astype(BF16)
    here, north = chip_y == col, core == 0
    size = own_r.shape[0]
    for a in range(2):
        for g in range(span // LANES):
            cut = slice(g * width, (g + 1) * width)
            same = slice(a * size + g * width, a * size + (g + 1) * width)
            flip = slice((1 - a) * size + g * width, (1 - a) * size + (g + 1) * width)
            from_0 = jnp.where(north, got[same, :], got_sib[same, :])
            from_1 = jnp.where(north, got_sib[flip, :], got[flip, :])
            local = jnp.where(core == a, own_r[cut, :], sib_r[cut, :])
            one = jnp.where(here, local, from_0).astype(F32)
            two = jnp.where(here, from_0, from_1).astype(F32)
            t0, t1 = jnp.where(own_first, one, two), jnp.where(own_first, two, one)
            for j4 in range(LANES // share):
                j = a * rows + g * (LANES // share) + j4
                tile = jnp.where(
                    group == 0, roll(t0, -share * j4),
                    jnp.where(group == 1, roll(t1, share - share * j4), 0.0),
                )
                rscr[pl.ds(j, width, stride=2 * block + PAD), :] = tile
                rscr[pl.ds(block + j, width, stride=2 * block + PAD), :] = roll(tile, HALF)
    left = lhs[...]
    for q in range(0, width, 2):
        at = [n * (LANES + PAD) for n in (q, q + 1)]
        rhs = jnp.concatenate([rscr[n : n + LANES, :] for n in at], axis=0).astype(BF16)
        prod = dot_nt(left, rhs).astype(BF16)
        for t in range(tiles):
            for e in range(2):
                mscr[t, (q + e) * width : (q + e + 1) * width, :] = prod[
                    t * width : (t + 1) * width, e * LANES : (e + 1) * LANES
                ]
    for t in range(0, tiles, 2):
        both = dot_nn(outer_wt[...], jnp.concatenate([mscr[t], mscr[t + 1]], axis=1))
        for e in range(2):
            update = both[:, e * LANES : (e + 1) * LANES] * (1.0 / total_rows)
            mid = (couple_t[t + e].astype(F32) + update).astype(BF16)
            mid_t[t + e] = mid
            x = mid.astype(F32)
            x = x - jnp.mean(x, axis=0, keepdims=True)
            x = x * lax.rsqrt(jnp.mean(x * x, axis=0, keepdims=True) + EPS)
            norm_t[t + e] = x.astype(BF16)


def right_body(norm_t, w_own, w_far, right_pk, gscr):
    gate_tiles(gscr, norm_t, w_own, w_far, 2)
    drop_pad(gscr, right_pk, 2 * norm_t.shape[0])


def left_body(norm_t, w_own, w_far, left_pk, gscr):
    gate_tiles(gscr, norm_t, w_own, w_far, 0)
    drop_pad(gscr, left_pk, 2 * norm_t.shape[0])


def close_body(norm_t, close_w, close_t):
    w_close = jnp.transpose(close_w[...].astype(F32)).astype(BF16)
    for t in range(norm_t.shape[0]):
        close_t[t] = jax.nn.sigmoid(dot_nn(w_close, norm_t[t]))


def triangle_body(rows, left_pk, own, sib, across, across_sib, *outs):
    mines, others = outs[: len(outs) // 2], outs[len(outs) // 2 :]
    n = rows // len(mines)
    col = lax.axis_index("col")
    row = lax.axis_index("row")
    chip_y, core = row // 2, row % 2
    is_low, here = core == 0, chip_y == col
    low = lane_of((rows, LANES)) < HALF

    def product(ch):
        cut = slice(ch * rows, (ch + 1) * rows)
        a = left_pk[cut, :]
        zero = jnp.zeros_like(a)
        lhs = jnp.concatenate([jnp.where(low, a, zero), jnp.where(low, zero, a)], axis=0)
        o, s, x, xs = own[cut, :], sib[cut, :], across[cut, :], across_sib[cut, :]
        n0, n1 = jnp.where(is_low, o, s), jnp.where(is_low, s, o)
        f0, f1 = jnp.where(is_low, x, xs), jnp.where(is_low, xs, x)
        rhs = jnp.concatenate(
            [
                jnp.where(here, n0, f0), jnp.where(here, n1, f1),
                jnp.where(here, f0, n0), jnp.where(here, f1, n1),
            ],
            axis=0,
        )
        prod = dot_nt(lhs, rhs)
        u, v = prod[:rows], prod[rows:]
        return jnp.where(low, u, roll(v, HALF)), jnp.where(low, roll(u, HALF), v)

    for ch in range(0, left_pk.shape[0] // rows, 2):
        (m0, o0), (m1, o1) = product(ch), product(ch + 1)
        to = slice(ch * n, (ch + 2) * n)
        for part in range(len(mines)):
            cut = slice(part * n, (part + 1) * n)
            mines[part][to, :] = jnp.concatenate([m0[cut], m1[cut]], axis=0)
            others[part][to, :] = jnp.concatenate([o0[cut], o1[cut]], axis=0).astype(BF16)


def final_body(n, first, count, *refs):
    refs = refs[1:] if first else refs
    halves, refs = refs[: 2 * count], refs[2 * count :]
    mid_t, close_t, final_w, out_h, scr, out, *sems = refs
    branch = lax.axis_index("branch")
    chans = halves[0].shape[0] // n
    low = lane_of((chans, LANES)) < HALF
    for k, half in enumerate(halves):
        scr[k] = half[...].astype(F32)
    owners = [branch, branch ^ 2, branch ^ 1, branch ^ 3]
    w_t = [final_w[pl.ds(pl.multiple_of(o * chans, chans), chans), :] for o in owners]
    w_t = jnp.transpose(jnp.concatenate(w_t, axis=0).astype(F32)).astype(BF16)
    per = n // 2
    base = first * per
    moves = []

    def normed(chunk, t):
        blocks = []
        for h in range(2):
            z0 = scr[2 * chunk + h, pl.ds(2 * t, chans, stride=n), :]
            z1 = scr[2 * chunk + h, pl.ds(2 * t + 1, chans, stride=n), :]
            blocks += [jnp.where(low, z0, roll(z1, HALF)), jnp.where(low, roll(z0, HALF), z1)]
        x = jnp.concatenate(blocks, axis=0)
        x = x - jnp.mean(x, axis=0, keepdims=True)
        x = x * lax.rsqrt(jnp.mean(x * x, axis=0, keepdims=True) + EPS)
        return x.astype(BF16)

    for chunk in range(count):
        for start in range(0, per, 2):
            change = dot_nn(
                w_t, jnp.concatenate([normed(chunk, start), normed(chunk, start + 1)], axis=1)
            )
            for e in range(2):
                t = chunk * per + start + e
                part_of = change[:, e * LANES : (e + 1) * LANES]
                result = mid_t[base + t].astype(F32) + close_t[base + t] * part_of
                out[t * LANES : (t + 1) * LANES, :] = jnp.transpose(result.astype(BF16))
        here = out.at[pl.ds(chunk * per * LANES, per * LANES)]
        there = out_h.at[pl.ds((base + chunk * per) * LANES, per * LANES)]
        moves.append(pltpu.make_async_copy(here, there, sems[chunk]))
        moves[-1].start()
    for move in moves:
        move.wait()


def attend_body(
    rows, head, query, gate, own, sib, across, across_sib, sent, got, w_out, *rest
):
    outs, (bscr, cscr) = rest[:-2], rest[-2:]
    col = lax.axis_index("col")
    row = lax.axis_index("row")
    branch = lax.axis_index("branch")
    top, is_low = row // 2 == 0, row % 2 == 0
    half = query.shape[0]
    scale = float(head) ** (-0.5)
    n_bias = bscr.shape[0] // 2
    start = sent.shape[0] - n_bias
    b_own, b_far = sent[start:, :].astype(F32), got[start:, :].astype(F32)
    b0, b1 = jnp.where(col == 0, b_own, b_far), jnp.where(col == 0, b_far, b_own)
    low = lane_of((n_bias, LANES)) < HALF
    bscr[pl.ds(0, n_bias, stride=2), :] = jnp.where(low, b0, roll(b1, HALF))
    bscr[pl.ds(1, n_bias, stride=2), :] = jnp.where(low, roll(b0, HALF), b1)
    bias = jnp.transpose(jnp.concatenate([bscr[...], bscr[...]], axis=0))
    b = [bias[n * rows : (n + 1) * rows] for n in range(LANES // rows)]
    b = [jnp.where(is_low, b[n], b[n ^ 1]) for n in range(len(b))]
    b = [jnp.where(top, b[n], b[n ^ 2]) for n in range(len(b))]
    bias = jnp.concatenate(b, axis=0)
    group = lane_of((rows, LANES)) // head

    def gather(at):
        cut = pl.ds(pl.multiple_of(at, rows), rows)
        return jnp.concatenate([own[cut, :], sib[cut, :], across[cut, :], across_sib[cut, :]], axis=0)

    batch = 4

    def some(step, carry):
        spots = [(step * batch + n) * rows for n in range(batch)]
        cuts = [pl.ds(pl.multiple_of(at, rows), rows) for at in spots]
        masked = []
        for cut in cuts:
            q = query[cut, :]
            zero = jnp.zeros_like(q)
            masked.append(
                jnp.concatenate(
                    [jnp.where(group == g, q, zero) for g in range(LANES // head)], axis=0
                )
            )
        scores = [dot_nt(gather(at), q) * scale + bias for at, q in zip(spots, masked)]
        tops = [jnp.max(x, axis=0, keepdims=True) for x in scores]
        expo = [jnp.exp(x - top) for x, top in zip(scores, tops)]
        expo = [x * (1.0 / jnp.sum(x, axis=0, keepdims=True)) for x in expo]
        full = [
            lax.dot_general(
                x.astype(BF16), gather(half + at), (((0,), (0,)), ((), ())),
                preferred_element_type=F32,
            )
            for x, at in zip(expo, spots)
        ]
        for cut, x in zip(cuts, full):
            ctx = x[:rows]
            for g in range(1, LANES // head):
                ctx = jnp.where(group == g, x[g * rows : (g + 1) * rows], ctx)
            cscr[cut, :] = (ctx * gate[cut, :]).astype(BF16)
        return carry

    lax.fori_loop(0, half // rows // batch, some, 0, unroll=True)
    ctx = cscr[...]
    low = lane_of((w_out.shape[0], LANES)) < HALF
    for m in range(len(outs)):
        chunk = branch ^ m
        at = pl.multiple_of((chunk // 2) * LANES, LANES)
        w = w_out[:, pl.ds(at, LANES)].astype(F32)
        w = jnp.where(chunk % 2 == 0, w, roll(w, HALF))
        w = jnp.concatenate([jnp.where(low, w, 0.0), jnp.where(low, 0.0, roll(w, HALF))], axis=0)
        outs[m][...] = dot_nn(ctx, w.astype(BF16)).astype(BF16)


def revise_body(hom, p0, p1, p2, p3, out):
    branch = lax.axis_index("branch")
    acc = p0[...].astype(F32) + p1[...].astype(F32)
    acc = acc + p2[...].astype(F32) + p3[...].astype(F32)
    n = acc.shape[0]
    at = pl.multiple_of((branch // 2) * LANES, LANES)
    base = hom[:, pl.ds(at, LANES)].astype(F32)
    base = jnp.where(branch % 2 == 0, base, roll(base, HALF))
    out[:n, :] = (acc + base[:n])[:, :HALF].astype(BF16)
    out[n:, :] = (roll(acc, HALF) + base[n:])[:, :HALF].astype(BF16)


def fast_per_device(
    mesh,
    homolog_tensor,
    couple_tensor,
    probe_matrix,
    lookup_matrix,
    content_matrix,
    scoring_sigmoid_matrix,
    scoring_final_matrix,
    couple_offset_matrix,
    product_first_matrix,
    product_second_matrix,
    product_final_matrix,
    trio_first_matrix,
    trio_second_matrix,
    trio_sigmoid_matrix,
    trio_final_matrix,
):
    n_b, n_r, n_c = (mesh.shape[a] for a in AXES)

    def send(x, source):
        pairs = []
        for b in range(n_b):
            for r in range(n_r):
                for c in range(n_c):
                    if (origin := source(b, r, c)) is not None:
                        sb, sr, sc = origin
                        pairs.append(((sb * n_r + sr) * n_c + sc, (b * n_r + r) * n_c + c))
        return lax.ppermute(x, AXES, pairs)

    def other_col(b, r, c):
        return b, r, c ^ 1

    def other_core(b, r, c):
        return b, r ^ 1, c

    def other_chip(b, r, c):
        return b, r ^ 2, c

    def turned(b, r, c):
        y, core = r // 2, r % 2
        if y == c:
            return None if core else (b, r, c ^ 1)
        return b, 2 * c + core, c ^ core

    share, rows, depth = homolog_tensor.shape
    block = couple_tensor.shape[1]
    chans = couple_tensor.shape[2]
    width = product_first_matrix.shape[1]
    heads_w = probe_matrix.shape[1]
    local_heads = couple_offset_matrix.shape[1]
    head = heads_w // local_heads
    quarter = trio_first_matrix.shape[2]
    tiles = rows * block // LANES
    n_rows = share * rows
    hom = homolog_tensor.reshape(n_rows, depth)
    couple = couple_tensor.reshape(rows * block, chans)

    flat = (n_rows * width // LANES, LANES)
    normed, left_t, right_t, couple_v, outer_w, offset_t, w_own = call(
        functools.partial(project_body, rows),
        [
            ((n_rows, depth), BF16), (flat, BF16), (flat, BF16),
            (couple.shape, BF16), (product_final_matrix.shape, BF16),
            ((local_heads, chans), BF16), ((4, quarter, chans), BF16),
        ],
        [
            ((depth // LANES, rows * (share + PAD), LANES), F32), ((n_rows, depth), BF16),
            ((width, depth), BF16), ((width, depth), BF16),
        ],
        sems=9,
        anywhere=8,
    )(
        hom, product_first_matrix.T, product_second_matrix.T, couple, product_final_matrix,
        couple_offset_matrix.T, jnp.transpose(trio_first_matrix, (0, 2, 1)),
        jnp.transpose(trio_second_matrix, (0, 2, 1)),
    )
    sib_r = send(right_t, other_core)
    got_r = send(jnp.concatenate([right_t, sib_r], axis=0), turned)
    couple_t, message, outer_wt = call(
        functools.partial(pair_body, width),
        [
            ((tiles, chans, LANES), BF16),
            ((flat[0] + local_heads * tiles, LANES), BF16),
            ((chans, width * width), BF16),
        ],
        [((local_heads * tiles, LANES), F32), ((width * (width + PAD), chans), F32)],
    )(couple_v, offset_t, outer_w, left_t)
    got = send(message, other_col)
    kv, query, gate = call(
        heads_body,
        [((n_rows, LANES), BF16), ((n_rows // 2, LANES), BF16), ((n_rows // 2, LANES), F32)],
    )(normed, lookup_matrix.T, content_matrix.T, probe_matrix.T, scoring_sigmoid_matrix.T)
    kv_x = send(kv, other_chip)
    kv_s = send(kv, other_core)
    kv_xs = send(kv_x, other_core)
    w_far = send(w_own, lambda b, r, c: (b ^ 2, r, c))
    got_rs = send(got_r, other_core)

    mid_t, norm_t = call(
        functools.partial(outer_body, share * n_c),
        [((tiles, chans, LANES), BF16), ((tiles, chans, LANES), BF16)],
        [
            ((tiles * width, LANES), BF16),
            ((width * (LANES + PAD), LANES), F32),
            ((tiles, width * width, LANES), BF16),
        ],
        mib=16,
    )(couple_t, outer_wt, message, got, right_t, sib_r, got_r, got_rs)
    (right_pk,) = call(
        right_body, [((quarter * rows, LANES), BF16)], [((quarter * (rows + PAD), LANES), F32)]
    )(norm_t, w_own, w_far)
    right_x = send(right_pk, other_chip)
    right_s = send(right_pk, other_core)
    (left_pk,) = call(
        left_body, [((quarter * rows, LANES), BF16)], [((quarter * (rows + PAD), LANES), F32)]
    )(norm_t, w_own, w_far)
    parts = call(
        functools.partial(attend_body, rows, head),
        [((n_rows // 2, LANES), BF16)] * n_b,
        [((local_heads * rows, LANES), F32), ((n_rows // 2, LANES), BF16)],
    )(query, gate, kv, kv_s, kv_x, kv_xs, message, got, scoring_final_matrix)
    right_xs = send(right_x, other_core)

    chunks = 4
    piece = (quarter * rows // chunks, LANES)
    products = call(
        functools.partial(triangle_body, rows), [(piece, F32)] * chunks + [(piece, BF16)] * chunks
    )(left_pk, right_pk, right_s, right_x, right_xs)
    mines = products[:chunks]
    fars = [send(x, other_col) for x in products[chunks:]]
    (close_t,) = call(close_body, [((tiles, chans, LANES), F32)])(norm_t, trio_sigmoid_matrix)
    parts = [parts[0]] + [send(parts[m], lambda b, r, c, m=m: (b ^ m, r, c)) for m in range(1, n_b)]
    half_own = [(mine + far.astype(F32)).astype(BF16) for mine, far in zip(mines, fars)]
    half_far = [send(half, lambda b, r, c: (b ^ 1, r, c)) for half in half_own]
    (revised,) = call(revise_body, [((n_rows, depth // n_b), BF16)])(hom, *parts)

    pair_out = ()
    for first, count in ((0, chunks // 2), (chunks // 2, chunks - chunks // 2)):
        ends = [x for k in range(first, first + count) for x in (half_own[k], half_far[k])]
        pair_out = call(
            functools.partial(final_body, rows // chunks, first, count),
            [((rows * block, chans), BF16)],
            [
                ((2 * count,) + piece, F32),
                ((rows * block * count // chunks, chans), BF16),
            ],
            mib=12,
            sems=count,
            out_hbm=1,
            anywhere=min(first, 1),
            alias={0: 0} if first else None,
        )(*pair_out, *ends, mid_t, close_t, trio_final_matrix)
    (pair_out,) = pair_out
    return (
        revised.reshape(share, rows, depth // n_b),
        pair_out.reshape(rows, block, chans),
    )


def fits(mesh, args):
    hom, couple = args[0], args[1]
    share, rows, depth = hom.shape
    return (
        mesh.shape["branch"] == 4
        and mesh.shape["row"] == 4
        and mesh.shape["col"] == 2
        and couple.shape[0] == rows
        and couple.shape[1] == 2 * rows == HALF
        and couple.shape[2] == LANES
        and share == QUART
        and args[2].shape[1] == HALF
        and depth == 4 * HALF
        and args[8].shape[1] == QUART
        and args[11].shape[2] == QUART
        and args[7].shape[1] == 2
    )


def dispatch(mesh, *args):
    if fits(mesh, args):
        return fast_per_device(mesh, *args)
    return plain_per_device(*args)


def solution(mesh):
    return jax.shard_map(
        functools.partial(dispatch, mesh),
        mesh=mesh,
        in_specs=(
            P("col", "row", None),
            P("row", "col", None),
            P(None, "branch"),
            P(None, "branch"),
            P(None, "branch"),
            P(None, "branch"),
            P("branch", None),
            P(None, "branch"),
            P(),
            P(),
            P(),
            P(None, None, "branch"),
            P(None, None, "branch"),
            P(),
            P(),
        ),
        out_specs=(P("col", "row", "branch"), P("row", "col", None)),
        check_vma=False,
    )
```

```python
import functools

import jax
import jax.numpy as jnp
from jax import lax
from jax.experimental import pallas as pl
from jax.experimental.pallas import tpu as pltpu
from jax.sharding import PartitionSpec as P


EPS = 1e-05


def spread_2(block, axis, owner):
    block = jnp.where(lax.axis_index(axis) == owner, block, jnp.zeros_like(block))
    return lax.psum(block, axis)


def standardise_rows(values):
    values = values.astype(jnp.float32)
    centred = values - jnp.mean(values, axis=-1, keepdims=True)
    variance = jnp.mean(centred * centred, axis=-1, keepdims=True)
    return centred / jnp.sqrt(variance + EPS)


def apply_linear(source, weights):
    return jnp.dot(
        source.reshape(-1, weights.shape[0]), weights, preferred_element_type=jnp.float32
    )


def attend(query, key, value, bias):
    scale = float(query.shape[-1]) ** (-0.5)
    scores = jnp.einsum("sihd,sjhd->shij", query, key, preferred_element_type=jnp.float32) * scale
    scores = scores + jnp.transpose(bias, (2, 0, 1)).astype(jnp.float32)[None]
    top = jnp.max(scores, axis=-1, keepdims=True)
    expo = jnp.exp(scores - top)
    total = jnp.sum(expo, axis=-1)
    summed = jnp.einsum(
        "shij,sjhd->sihd", expo.astype(jnp.bfloat16), value, preferred_element_type=jnp.float32
    )
    return summed / jnp.transpose(total, (0, 2, 1))[..., None]


def plain_per_device(
    homolog_tensor,
    couple_tensor,
    probe_matrix,
    lookup_matrix,
    content_matrix,
    scoring_sigmoid_matrix,
    scoring_final_matrix,
    couple_offset_matrix,
    product_first_matrix,
    product_second_matrix,
    product_final_matrix,
    trio_first_matrix,
    trio_second_matrix,
    trio_sigmoid_matrix,
    trio_final_matrix,
):
    branches = lax.axis_size("branch")
    rows_count = lax.axis_size("row")
    cols_count = lax.axis_size("col")
    quadrant_share = lax.axis_index("branch")
    col_index = lax.axis_index("col")
    homolog_share, position_tile, channel_extent = homolog_tensor.shape
    c_block = couple_tensor.shape[1]
    residues = position_tile * rows_count
    depth = probe_matrix.shape[1]
    local_heads = couple_offset_matrix.shape[1]
    head_size = depth // local_heads
    q_rows = position_tile // branches
    total_rows = homolog_share * cols_count
    outer_width = product_first_matrix.shape[1]
    standardised_tensor = standardise_rows(homolog_tensor).astype(jnp.bfloat16)
    pair_normed = standardise_rows(couple_tensor).astype(jnp.bfloat16)
    bias_tile = (
        apply_linear(pair_normed, couple_offset_matrix)
        .astype(jnp.bfloat16)
        .reshape(position_tile, c_block, local_heads)
    )
    bias_band = lax.all_gather(bias_tile, "col", axis=1, tiled=True)
    spread = lax.all_to_all(standardised_tensor, "row", split_axis=0, concat_axis=1, tiled=True)
    few = spread.shape[0]
    shaped = (few, residues, local_heads, head_size)
    query = apply_linear(spread, probe_matrix).astype(jnp.bfloat16).reshape(shaped)
    key = apply_linear(spread, lookup_matrix).astype(jnp.bfloat16).reshape(shaped)
    value = apply_linear(spread, content_matrix).astype(jnp.bfloat16).reshape(shaped)
    gate_pre = apply_linear(spread, scoring_sigmoid_matrix).reshape(shaped)
    bias_full = lax.all_gather(bias_band, "row", axis=0, tiled=True)
    attended_values = attend(query, key, value, bias_full) * jax.nn.sigmoid(gate_pre)
    attended_values = attended_values.astype(jnp.bfloat16).reshape(few, residues, depth)
    attended_values = lax.all_to_all(
        attended_values, "row", split_axis=1, concat_axis=0, tiled=True
    )
    joined_tensor = apply_linear(attended_values, scoring_final_matrix).reshape(
        homolog_share, position_tile, channel_extent
    )
    joined_tensor = lax.psum_scatter(
        joined_tensor.astype(jnp.bfloat16), "branch", scatter_dimension=2, tiled=True
    ).astype(jnp.float32)
    device_share = channel_extent // branches
    local_alignment = lax.dynamic_slice_in_dim(
        homolog_tensor, quadrant_share * device_share, device_share, 2
    )
    revised_homolog_matrix = (local_alignment.astype(jnp.float32) + joined_tensor).astype(
        jnp.bfloat16
    )
    left_rows = lax.dynamic_slice_in_dim(standardised_tensor, quadrant_share * q_rows, q_rows, 1)
    left_outer = (
        apply_linear(left_rows, product_first_matrix)
        .astype(jnp.bfloat16)
        .reshape(homolog_share, q_rows * outer_width)
    )
    right_local = (
        apply_linear(standardised_tensor, product_second_matrix)
        .astype(jnp.bfloat16)
        .reshape(homolog_share, position_tile, outer_width)
    )
    right_outer = lax.all_gather(right_local, "row", axis=1, tiled=True)
    wide_out = product_final_matrix.astype(jnp.float32)
    left_major = jnp.transpose(left_outer)
    count = lax.axis_size("col") * c_block
    piece = right_outer.reshape(homolog_share, count * outer_width)
    outer = jnp.dot(left_major, piece, preferred_element_type=jnp.float32)
    outer = outer.reshape(q_rows, outer_width, count, outer_width)
    outer = jnp.transpose(outer, (2, 0, 1, 3)).reshape(count * q_rows, outer_width * outer_width)
    term = jnp.dot(outer, wide_out, precision=lax.Precision.HIGHEST) / total_rows
    update = lax.psum_scatter(
        term.reshape(count, q_rows, wide_out.shape[1]).astype(jnp.bfloat16),
        "col",
        scatter_dimension=0,
        tiled=True,
    ).astype(jnp.float32)
    update = jnp.transpose(update, (1, 0, 2))
    pair_rows = lax.dynamic_slice_in_dim(couple_tensor, quadrant_share * q_rows, q_rows, 0)
    mid_rows = (pair_rows.astype(jnp.float32) + update).astype(jnp.bfloat16)
    pair_mid = lax.all_gather(mid_rows, "branch", axis=0, tiled=True)
    tri_normed = standardise_rows(pair_mid).astype(jnp.bfloat16)

    def gated(weights):
        linear = apply_linear(tri_normed, weights[0])
        opening = apply_linear(tri_normed, weights[1])
        return (
            (jax.nn.sigmoid(opening) * linear)
            .astype(jnp.bfloat16)
            .reshape(position_tile, c_block, weights.shape[2])
        )

    tri_left = gated(trio_first_matrix)
    tri_right = gated(trio_second_matrix)
    left_band, right_band = (
        lax.all_gather(tri_left, "col", axis=1, tiled=True),
        lax.all_gather(tri_right, "col", axis=1, tiled=True),
    )
    ratio = rows_count // cols_count

    def mirror(offset):
        return spread_2(right_band, "row", col_index * ratio + offset)

    right_cols = jnp.concatenate([mirror(offset) for offset in range(ratio)], axis=0)
    product = jnp.einsum("ikc,jkc->ijc", left_band, right_cols, preferred_element_type=jnp.float32)
    product = lax.all_to_all(product, "branch", split_axis=0, concat_axis=2, tiled=True)
    product_normed = standardise_rows(product).astype(jnp.bfloat16)
    own_normed = lax.dynamic_slice_in_dim(tri_normed, quadrant_share * q_rows, q_rows, 0)
    closing = jax.nn.sigmoid(apply_linear(own_normed, trio_sigmoid_matrix)).reshape(
        q_rows, c_block, -1
    )
    change = apply_linear(product_normed, trio_final_matrix).reshape(q_rows, c_block, -1)
    out_rows = (mid_rows.astype(jnp.float32) + closing * change).astype(jnp.bfloat16)
    pairwise_output = lax.all_gather(out_rows, "branch", axis=0, tiled=True)
    return (revised_homolog_matrix, pairwise_output)


F32 = jnp.float32
BF16 = jnp.bfloat16
AXES = ("branch", "row", "col")
LANES = 128
HALF = LANES // 2
QUART = LANES // 4
PAD = 8


def lane_of(shape):
    return lax.broadcasted_iota(jnp.int32, shape, len(shape) - 1)


def roll(x, shift):
    shift %= x.shape[-1]
    return pltpu.roll(x, shift, x.ndim - 1) if shift else x


def dot_nn(a, b):
    return jnp.dot(a, b, preferred_element_type=F32)


def dot_nt(a, b):
    return lax.dot_general(a, b, (((1,), (1,)), ((), ())), preferred_element_type=F32)


def call(body, outs, scratch=(), flops=10**6, mib=8, sems=0, anywhere=0, out_hbm=0, alias=None):
    scratch = [pltpu.VMEM(s, d) for s, d in scratch]
    scratch += [pltpu.SemaphoreType.DMA] * sems
    far, near = pl.BlockSpec(memory_space=pltpu.HBM), pl.BlockSpec(memory_space=pltpu.VMEM)

    def run(*args):
        specs = {}
        if anywhere:
            specs["in_specs"] = [far] * anywhere + [near] * (len(args) - anywhere)
        if out_hbm:
            specs["out_specs"] = (far,) * out_hbm
        args = [
            pltpu.with_memory_space_constraint(x, pltpu.HBM) if n < anywhere else x
            for n, x in enumerate(args)
        ]
        return pl.pallas_call(
            body,
            out_shape=tuple(jax.ShapeDtypeStruct(s, d) for s, d in outs),
            scratch_shapes=scratch,
            compiler_params=pltpu.CompilerParams(vmem_limit_bytes=mib * 2**20),
            cost_estimate=pl.CostEstimate(flops=flops, bytes_accessed=2**19, transcendentals=0),
            input_output_aliases=alias or {},
            **specs,
        )(*args)

    return run


def project_body(
    rows, hom_h, left_h, right_h, couple_h, outer_h, offset_h, first_h, second_h,
    normed, left_t, right_t, couple, outer_w, offset, gates_w, scr, hom, left_w, right_w, *sems,
):
    parts = 2
    cut = hom.shape[0] // parts
    pieces = [pl.ds(n * cut, cut) for n in range(parts)]
    pairs = [(hom_h.at[p], hom.at[p]) for p in pieces]
    pairs += [(left_h, left_w), (right_h, right_w), (couple_h, couple), (outer_h, outer_w)]
    pairs += [(offset_h, offset), (first_h, gates_w.at[pl.ds(0, 2)])]
    pairs += [(second_h, gates_w.at[pl.ds(2, 2)])]
    moves = [pltpu.make_async_copy(src, dst, sem) for (src, dst), sem in zip(pairs, sems)]
    for move in moves[: parts + 2]:
        move.start()
    n_rows, depth = hom.shape
    share = n_rows // rows
    width = left_w.shape[0]
    step = 2
    for first in range(0, share, step):
        if first * rows % cut == 0:
            moves[first * rows // cut].wait()
        if first == 0:
            for move in moves[parts + 2 :]:
                move.start()
        x = hom[first * rows : (first + step) * rows, :].astype(F32)
        x = x - jnp.mean(x, axis=-1, keepdims=True)
        x = x * lax.rsqrt(jnp.mean(x * x, axis=-1, keepdims=True) + EPS)
        normed[first * rows : (first + step) * rows, :] = x.astype(BF16)
        for s in range(step):
            piece = x[s * rows : (s + 1) * rows, :]
            for part in range(depth // LANES):
                scr[part, pl.ds(first + s, rows, stride=share + PAD), :] = piece[
                    :, part * LANES : (part + 1) * LANES
                ]
    moves[parts].wait()
    moves[parts + 1].wait()
    weights = jnp.concatenate([left_w[...], right_w[...]], axis=0)
    acc = 0
    for part in range(depth // LANES):
        x = [scr[part, i * (share + PAD) : i * (share + PAD) + share, :] for i in range(rows)]
        x = jnp.concatenate(x, axis=0).astype(BF16)
        acc = acc + dot_nt(weights[:, part * LANES : (part + 1) * LANES], x)
    for g in range(n_rows // LANES):
        cut = slice(g * LANES, (g + 1) * LANES)
        left_t[g * width : (g + 1) * width, :] = acc[:width, cut].astype(BF16)
        right_t[g * width : (g + 1) * width, :] = acc[width:, cut].astype(BF16)
    for move in moves[parts + 2 :]:
        move.wait()


def heads_body(normed, key_w, value_w, query_w, gate_w, kv, query, gate):
    half = normed.shape[0] // 2
    x = normed[...]
    low = lane_of((half, LANES)) < HALF

    weights = [w[...] for w in (key_w, value_w, query_w, gate_w)]
    full = dot_nt(x, jnp.concatenate(weights, axis=0))

    def both(y):
        top, bottom = y[:half], y[half:]
        return (
            jnp.where(low, top, roll(bottom, HALF)),
            jnp.where(low, roll(top, HALF), bottom),
        )

    k, v = both(full[:, :LANES])
    kv[:half, :] = k.astype(BF16)
    kv[half:, :] = v.astype(BF16)
    q, g = both(full[:, LANES:])
    query[...] = q.astype(BF16)
    gate[...] = jax.nn.sigmoid(g)


def pair_body(width, couple, offset_t, outer_w, left_t, couple_t, message, outer_wt, scr, wscr):
    tiles = couple.shape[0] // LANES
    for t in range(tiles):
        x = jnp.transpose(couple[t * LANES : (t + 1) * LANES, :])
        couple_t[t] = x
        x = x.astype(F32)
        x = x - jnp.mean(x, axis=0, keepdims=True)
        x = x * lax.rsqrt(jnp.mean(x * x, axis=0, keepdims=True) + EPS)
        scr[pl.ds(t, offset_t.shape[0], stride=tiles), :] = dot_nn(offset_t[...], x.astype(BF16))
    span = left_t.shape[0]
    message[:span, :] = left_t[...]
    message[span:, :] = scr[...].astype(BF16)
    per = LANES // width
    for p in range(width):
        cut = slice(p * width, (p + 1) * width)
        wscr[p * (width + PAD) : p * (width + PAD) + width, :] = outer_w[cut, :].astype(F32)
    for g in range(width // per):
        block = jnp.concatenate(
            [wscr[pl.ds(g * per + q, width, stride=width + PAD), :] for q in range(per)], axis=0
        )
        outer_wt[:, g * LANES : (g + 1) * LANES] = jnp.transpose(block.astype(BF16))


def gate_tiles(scr, norm_t, w_own, w_far, first):
    tiles = norm_t.shape[0]
    weights = jnp.concatenate(
        [w_own[first], w_far[first], w_own[first + 1], w_far[first + 1]], axis=0
    )
    half = weights.shape[0] // 2
    for t in range(0, tiles, 2):
        y = dot_nn(weights, jnp.concatenate([norm_t[t], norm_t[t + 1]], axis=1))
        gated = jax.nn.sigmoid(y[half:]) * y[:half]
        store_gated(scr, t, 2 * tiles + PAD, gated[:, :LANES])
        store_gated(scr, t + 1, 2 * tiles + PAD, gated[:, LANES:])


def drop_pad(scr, out, rows):
    for n in range(out.shape[0] // rows):
        at = n * (rows + PAD)
        out[n * rows : (n + 1) * rows, :] = scr[at : at + rows, :].astype(out.dtype)


def store_gated(scr, t, rows, gated):
    chans = gated.shape[0] // 2
    low = lane_of((chans, LANES)) < HALF
    a, b = gated[:chans], gated[chans:]
    scr[pl.ds(2 * t, chans, stride=rows), :] = jnp.where(low, a, roll(b, HALF))
    scr[pl.ds(2 * t + 1, chans, stride=rows), :] = jnp.where(low, roll(a, HALF), b)


def outer_body(
    total_rows, couple_t, outer_wt, left_own, left_far, own_r, sib_r, got, got_sib,
    mid_t, norm_t, lhs, rscr, mscr,
):
    col = lax.axis_index("col")
    row = lax.axis_index("row")
    chip_y, core = row // 2, row % 2
    width = lhs.shape[0] // couple_t.shape[0]
    span = own_r.shape[0] // width * LANES
    tiles = couple_t.shape[0]
    rows = 2 * tiles
    share = span // rows
    block = rows * 2
    group = lane_of((width, LANES)) // share
    own_first = col == 0
    for g in range(span // LANES):
        cut = slice(g * width, (g + 1) * width)
        own, far = left_own[cut, :].astype(F32), left_far[cut, :].astype(F32)
        a, b = jnp.where(own_first, own, far), jnp.where(own_first, far, own)
        even = jnp.where(
            group == 0, a,
            jnp.where(group == 1, roll(b, QUART), jnp.where(group == 2, roll(a, QUART), roll(b, HALF))),
        )
        odd = jnp.where(
            group == 0, roll(a, HALF),
            jnp.where(group == 1, roll(b, -QUART), jnp.where(group == 2, roll(a, -QUART), b)),
        )
        lhs[2 * g * width : (2 * g + 1) * width, :] = even.astype(BF16)
        lhs[(2 * g + 1) * width : (2 * g + 2) * width, :] = odd.astype(BF16)
    here, north = chip_y == col, core == 0
    size = own_r.shape[0]
    for a in range(2):
        for g in range(span // LANES):
            cut = slice(g * width, (g + 1) * width)
            same = slice(a * size + g * width, a * size + (g + 1) * width)
            flip = slice((1 - a) * size + g * width, (1 - a) * size + (g + 1) * width)
            from_0 = jnp.where(north, got[same, :], got_sib[same, :])
            from_1 = jnp.where(north, got_sib[flip, :], got[flip, :])
            local = jnp.where(core == a, own_r[cut, :], sib_r[cut, :])
            one = jnp.where(here, local, from_0).astype(F32)
            two = jnp.where(here, from_0, from_1).astype(F32)
            t0, t1 = jnp.where(own_first, one, two), jnp.where(own_first, two, one)
            for j4 in range(LANES // share):
                j = a * rows + g * (LANES // share) + j4
                tile = jnp.where(
                    group == 0, roll(t0, -share * j4),
                    jnp.where(group == 1, roll(t1, share - share * j4), 0.0),
                )
                rscr[pl.ds(j, width, stride=2 * block + PAD), :] = tile
                rscr[pl.ds(block + j, width, stride=2 * block + PAD), :] = roll(tile, HALF)
    left = lhs[...]
    for q in range(0, width, 2):
        at = [n * (LANES + PAD) for n in (q, q + 1)]
        rhs = jnp.concatenate([rscr[n : n + LANES, :] for n in at], axis=0).astype(BF16)
        prod = dot_nt(left, rhs).astype(BF16)
        for t in range(tiles):
            for e in range(2):
                mscr[t, (q + e) * width : (q + e + 1) * width, :] = prod[
                    t * width : (t + 1) * width, e * LANES : (e + 1) * LANES
                ]
    for t in range(0, tiles, 2):
        both = dot_nn(outer_wt[...], jnp.concatenate([mscr[t], mscr[t + 1]], axis=1))
        for e in range(2):
            update = both[:, e * LANES : (e + 1) * LANES] * (1.0 / total_rows)
            mid = (couple_t[t + e].astype(F32) + update).astype(BF16)
            mid_t[t + e] = mid
            x = mid.astype(F32)
            x = x - jnp.mean(x, axis=0, keepdims=True)
            x = x * lax.rsqrt(jnp.mean(x * x, axis=0, keepdims=True) + EPS)
            norm_t[t + e] = x.astype(BF16)


def right_body(norm_t, w_own, w_far, right_pk, gscr):
    gate_tiles(gscr, norm_t, w_own, w_far, 2)
    drop_pad(gscr, right_pk, 2 * norm_t.shape[0])


def left_body(norm_t, w_own, w_far, left_pk, gscr):
    gate_tiles(gscr, norm_t, w_own, w_far, 0)
    drop_pad(gscr, left_pk, 2 * norm_t.shape[0])


def close_body(norm_t, close_w, close_t):
    w_close = jnp.transpose(close_w[...].astype(F32)).astype(BF16)
    for t in range(norm_t.shape[0]):
        close_t[t] = jax.nn.sigmoid(dot_nn(w_close, norm_t[t]))


def triangle_body(rows, part, left_pk, own, sib, across, across_sib, mine, other):
    col = lax.axis_index("col")
    row = lax.axis_index("row")
    chip_y, core = row // 2, row % 2
    is_low, here = core == 0, chip_y == col
    n = rows // 2
    low = lane_of((n, LANES)) < HALF
    for ch in range(left_pk.shape[0] // rows):
        cut = slice(ch * rows, (ch + 1) * rows)
        a = left_pk[ch * rows + part * n : ch * rows + (part + 1) * n, :]
        zero = jnp.zeros_like(a)
        lhs = jnp.concatenate([jnp.where(low, a, zero), jnp.where(low, zero, a)], axis=0)
        o, s, x, xs = own[cut, :], sib[cut, :], across[cut, :], across_sib[cut, :]
        n0, n1 = jnp.where(is_low, o, s), jnp.where(is_low, s, o)
        f0, f1 = jnp.where(is_low, x, xs), jnp.where(is_low, xs, x)
        rhs = jnp.concatenate(
            [
                jnp.where(here, n0, f0), jnp.where(here, n1, f1),
                jnp.where(here, f0, n0), jnp.where(here, f1, n1),
            ],
            axis=0,
        )
        prod = dot_nt(lhs, rhs)
        u, v = prod[:n], prod[n:]
        to = slice(ch * n, (ch + 1) * n)
        mine[to, :] = jnp.where(low, u, roll(v, HALF))
        other[to, :] = jnp.where(low, roll(u, HALF), v).astype(BF16)


def final_body(n, part, *refs):
    half_own, half_far, mid_t, close_t, final_w, out_h, scr, out, *sems = refs[part:]
    branch = lax.axis_index("branch")
    chans = half_own.shape[0] // n
    low = lane_of((chans, LANES)) < HALF
    for h, half in enumerate((half_own, half_far)):
        for c in range(chans):
            scr[h, c * (n + PAD) : c * (n + PAD) + n, :] = half[c * n : (c + 1) * n, :].astype(F32)
    owners = [branch, branch ^ 2, branch ^ 1, branch ^ 3]
    w_t = [final_w[pl.ds(pl.multiple_of(o * chans, chans), chans), :] for o in owners]
    w_t = jnp.transpose(jnp.concatenate(w_t, axis=0).astype(F32)).astype(BF16)
    tiles = n // 2
    per = tiles // len(sems)
    base = part * tiles
    moves = []

    def normed(t):
        blocks = []
        for h in range(2):
            z0 = scr[h, pl.ds(2 * t, chans, stride=n + PAD), :]
            z1 = scr[h, pl.ds(2 * t + 1, chans, stride=n + PAD), :]
            blocks += [jnp.where(low, z0, roll(z1, HALF)), jnp.where(low, roll(z0, HALF), z1)]
        x = jnp.concatenate(blocks, axis=0)
        x = x - jnp.mean(x, axis=0, keepdims=True)
        x = x * lax.rsqrt(jnp.mean(x * x, axis=0, keepdims=True) + EPS)
        return x.astype(BF16)

    for start in range(0, tiles, per):
        change = dot_nn(
            w_t, jnp.concatenate([normed(t) for t in range(start, start + per)], axis=1)
        )
        for e in range(per):
            t = start + e
            part_of = change[:, e * LANES : (e + 1) * LANES]
            result = mid_t[base + t].astype(F32) + close_t[base + t] * part_of
            out[t * LANES : (t + 1) * LANES, :] = jnp.transpose(result.astype(BF16))
        here = out.at[pl.ds(start * LANES, per * LANES)]
        there = out_h.at[pl.ds((base + start) * LANES, per * LANES)]
        moves.append(pltpu.make_async_copy(here, there, sems[start // per]))
        moves[-1].start()
    for move in moves:
        move.wait()


def attend_body(
    rows, head, query, gate, own, sib, across, across_sib, sent, got, w_out, *rest
):
    outs, (bscr, cscr) = rest[:-2], rest[-2:]
    col = lax.axis_index("col")
    row = lax.axis_index("row")
    branch = lax.axis_index("branch")
    top, is_low = row // 2 == 0, row % 2 == 0
    half = query.shape[0]
    scale = float(head) ** (-0.5)
    n_bias = bscr.shape[0] // 2
    start = sent.shape[0] - n_bias
    b_own, b_far = sent[start:, :].astype(F32), got[start:, :].astype(F32)
    b0, b1 = jnp.where(col == 0, b_own, b_far), jnp.where(col == 0, b_far, b_own)
    low = lane_of((n_bias, LANES)) < HALF
    bscr[pl.ds(0, n_bias, stride=2), :] = jnp.where(low, b0, roll(b1, HALF))
    bscr[pl.ds(1, n_bias, stride=2), :] = jnp.where(low, roll(b0, HALF), b1)
    bias = jnp.transpose(jnp.concatenate([bscr[...], bscr[...]], axis=0))
    b = [bias[n * rows : (n + 1) * rows] for n in range(LANES // rows)]
    b = [jnp.where(is_low, b[n], b[n ^ 1]) for n in range(len(b))]
    b = [jnp.where(top, b[n], b[n ^ 2]) for n in range(len(b))]
    bias = jnp.concatenate(b, axis=0)
    group = lane_of((rows, LANES)) // head

    def gather(at):
        cut = pl.ds(pl.multiple_of(at, rows), rows)
        return jnp.concatenate([own[cut, :], sib[cut, :], across[cut, :], across_sib[cut, :]], axis=0)

    batch = 4

    def some(step, carry):
        spots = [(step * batch + n) * rows for n in range(batch)]
        cuts = [pl.ds(pl.multiple_of(at, rows), rows) for at in spots]
        masked = []
        for cut in cuts:
            q = query[cut, :]
            zero = jnp.zeros_like(q)
            masked.append(
                jnp.concatenate(
                    [jnp.where(group == g, q, zero) for g in range(LANES // head)], axis=0
                )
            )
        scores = [dot_nt(gather(at), q) * scale + bias for at, q in zip(spots, masked)]
        tops = [jnp.max(x, axis=0, keepdims=True) for x in scores]
        expo = [jnp.exp(x - top) for x, top in zip(scores, tops)]
        expo = [x * (1.0 / jnp.sum(x, axis=0, keepdims=True)) for x in expo]
        full = [
            lax.dot_general(
                x.astype(BF16), gather(half + at), (((0,), (0,)), ((), ())),
                preferred_element_type=F32,
            )
            for x, at in zip(expo, spots)
        ]
        for cut, x in zip(cuts, full):
            ctx = x[:rows]
            for g in range(1, LANES // head):
                ctx = jnp.where(group == g, x[g * rows : (g + 1) * rows], ctx)
            cscr[cut, :] = (ctx * gate[cut, :]).astype(BF16)
        return carry

    lax.fori_loop(0, half // rows // batch, some, 0, unroll=True)
    ctx = cscr[...]
    low = lane_of((w_out.shape[0], LANES)) < HALF
    for m in range(len(outs)):
        chunk = branch ^ m
        at = pl.multiple_of((chunk // 2) * LANES, LANES)
        w = w_out[:, pl.ds(at, LANES)].astype(F32)
        w = jnp.where(chunk % 2 == 0, w, roll(w, HALF))
        w = jnp.concatenate([jnp.where(low, w, 0.0), jnp.where(low, 0.0, roll(w, HALF))], axis=0)
        outs[m][...] = dot_nn(ctx, w.astype(BF16)).astype(BF16)


def revise_body(hom, p0, p1, p2, p3, out):
    branch = lax.axis_index("branch")
    acc = p0[...].astype(F32) + p1[...].astype(F32)
    acc = acc + p2[...].astype(F32) + p3[...].astype(F32)
    n = acc.shape[0]
    at = pl.multiple_of((branch // 2) * LANES, LANES)
    base = hom[:, pl.ds(at, LANES)].astype(F32)
    base = jnp.where(branch % 2 == 0, base, roll(base, HALF))
    out[:n, :] = (acc + base[:n])[:, :HALF].astype(BF16)
    out[n:, :] = (roll(acc, HALF) + base[n:])[:, :HALF].astype(BF16)


def fast_per_device(
    mesh,
    homolog_tensor,
    couple_tensor,
    probe_matrix,
    lookup_matrix,
    content_matrix,
    scoring_sigmoid_matrix,
    scoring_final_matrix,
    couple_offset_matrix,
    product_first_matrix,
    product_second_matrix,
    product_final_matrix,
    trio_first_matrix,
    trio_second_matrix,
    trio_sigmoid_matrix,
    trio_final_matrix,
):
    n_b, n_r, n_c = (mesh.shape[a] for a in AXES)

    def send(x, source):
        pairs = []
        for b in range(n_b):
            for r in range(n_r):
                for c in range(n_c):
                    if (origin := source(b, r, c)) is not None:
                        sb, sr, sc = origin
                        pairs.append(((sb * n_r + sr) * n_c + sc, (b * n_r + r) * n_c + c))
        return lax.ppermute(x, AXES, pairs)

    def other_col(b, r, c):
        return b, r, c ^ 1

    def other_core(b, r, c):
        return b, r ^ 1, c

    def other_chip(b, r, c):
        return b, r ^ 2, c

    def turned(b, r, c):
        y, core = r // 2, r % 2
        if y == c:
            return None if core else (b, r, c ^ 1)
        return b, 2 * c + core, c ^ core

    share, rows, depth = homolog_tensor.shape
    block = couple_tensor.shape[1]
    chans = couple_tensor.shape[2]
    width = product_first_matrix.shape[1]
    heads_w = probe_matrix.shape[1]
    local_heads = couple_offset_matrix.shape[1]
    head = heads_w // local_heads
    quarter = trio_first_matrix.shape[2]
    tiles = rows * block // LANES
    n_rows = share * rows
    hom = homolog_tensor.reshape(n_rows, depth)
    couple = couple_tensor.reshape(rows * block, chans)

    flat = (n_rows * width // LANES, LANES)
    normed, left_t, right_t, couple_v, outer_w, offset_t, w_own = call(
        functools.partial(project_body, rows),
        [
            ((n_rows, depth), BF16), (flat, BF16), (flat, BF16),
            (couple.shape, BF16), (product_final_matrix.shape, BF16),
            ((local_heads, chans), BF16), ((4, quarter, chans), BF16),
        ],
        [
            ((depth // LANES, rows * (share + PAD), LANES), F32), ((n_rows, depth), BF16),
            ((width, depth), BF16), ((width, depth), BF16),
        ],
        sems=9,
        anywhere=8,
    )(
        hom, product_first_matrix.T, product_second_matrix.T, couple, product_final_matrix,
        couple_offset_matrix.T, jnp.transpose(trio_first_matrix, (0, 2, 1)),
        jnp.transpose(trio_second_matrix, (0, 2, 1)),
    )
    sib_r = send(right_t, other_core)
    got_r = send(jnp.concatenate([right_t, sib_r], axis=0), turned)
    couple_t, message, outer_wt = call(
        functools.partial(pair_body, width),
        [
            ((tiles, chans, LANES), BF16),
            ((flat[0] + local_heads * tiles, LANES), BF16),
            ((chans, width * width), BF16),
        ],
        [((local_heads * tiles, LANES), F32), ((width * (width + PAD), chans), F32)],
    )(couple_v, offset_t, outer_w, left_t)
    got = send(message, other_col)
    kv, query, gate = call(
        heads_body,
        [((n_rows, LANES), BF16), ((n_rows // 2, LANES), BF16), ((n_rows // 2, LANES), F32)],
    )(normed, lookup_matrix.T, content_matrix.T, probe_matrix.T, scoring_sigmoid_matrix.T)
    kv_x = send(kv, other_chip)
    kv_s = send(kv, other_core)
    kv_xs = send(kv_x, other_core)
    w_far = send(w_own, lambda b, r, c: (b ^ 2, r, c))
    got_rs = send(got_r, other_core)

    mid_t, norm_t = call(
        functools.partial(outer_body, share * n_c),
        [((tiles, chans, LANES), BF16), ((tiles, chans, LANES), BF16)],
        [
            ((tiles * width, LANES), BF16),
            ((width * (LANES + PAD), LANES), F32),
            ((tiles, width * width, LANES), BF16),
        ],
        mib=16,
    )(couple_t, outer_wt, message, got, right_t, sib_r, got_r, got_rs)
    (right_pk,) = call(
        right_body, [((quarter * rows, LANES), BF16)], [((quarter * (rows + PAD), LANES), F32)]
    )(norm_t, w_own, w_far)
    right_x = send(right_pk, other_chip)
    right_s = send(right_pk, other_core)
    (left_pk,) = call(
        left_body, [((quarter * rows, LANES), BF16)], [((quarter * (rows + PAD), LANES), F32)]
    )(norm_t, w_own, w_far)
    parts = call(
        functools.partial(attend_body, rows, head),
        [((n_rows // 2, LANES), BF16)] * n_b,
        [((local_heads * rows, LANES), F32), ((n_rows // 2, LANES), BF16)],
    )(query, gate, kv, kv_s, kv_x, kv_xs, message, got, scoring_final_matrix)
    right_xs = send(right_x, other_core)

    mines, fars = [], []
    for part in range(2):
        mine, other = call(
            functools.partial(triangle_body, rows, part),
            [((quarter * rows // 2, LANES), F32), ((quarter * rows // 2, LANES), BF16)],
        )(left_pk, right_pk, right_s, right_x, right_xs)
        mines.append(mine)
        fars.append(send(other, other_col))
    (close_t,) = call(close_body, [((tiles, chans, LANES), F32)])(norm_t, trio_sigmoid_matrix)
    parts = [parts[0]] + [send(parts[m], lambda b, r, c, m=m: (b ^ m, r, c)) for m in range(1, n_b)]
    half_own = [(mine + far.astype(F32)).astype(BF16) for mine, far in zip(mines, fars)]
    half_far = [send(half, lambda b, r, c: (b ^ 1, r, c)) for half in half_own]
    (revised,) = call(revise_body, [((n_rows, depth // n_b), BF16)])(hom, *parts)

    pair_out = ()
    for part in range(2):
        pair_out = call(
            functools.partial(final_body, rows // 2, part),
            [((rows * block, chans), BF16)],
            [((2, quarter * (rows // 2 + PAD), LANES), F32), ((rows * block // 2, chans), BF16)],
            mib=12,
            sems=4,
            out_hbm=1,
            anywhere=part,
            alias={0: 0} if part else None,
        )(*pair_out, half_own[part], half_far[part], mid_t, close_t, trio_final_matrix)
    (pair_out,) = pair_out
    return (
        revised.reshape(share, rows, depth // n_b),
        pair_out.reshape(rows, block, chans),
    )


def fits(mesh, args):
    hom, couple = args[0], args[1]
    share, rows, depth = hom.shape
    return (
        mesh.shape["branch"] == 4
        and mesh.shape["row"] == 4
        and mesh.shape["col"] == 2
        and couple.shape[0] == rows
        and couple.shape[1] == 2 * rows == HALF
        and couple.shape[2] == LANES
        and share == QUART
        and args[2].shape[1] == HALF
        and depth == 4 * HALF
        and args[8].shape[1] == QUART
        and args[11].shape[2] == QUART
        and args[7].shape[1] == 2
    )


def dispatch(mesh, *args):
    if fits(mesh, args):
        return fast_per_device(mesh, *args)
    return plain_per_device(*args)


def solution(mesh):
    return jax.shard_map(
        functools.partial(dispatch, mesh),
        mesh=mesh,
        in_specs=(
            P("col", "row", None),
            P("row", "col", None),
            P(None, "branch"),
            P(None, "branch"),
            P(None, "branch"),
            P(None, "branch"),
            P("branch", None),
            P(None, "branch"),
            P(),
            P(),
            P(),
            P(None, None, "branch"),
            P(None, None, "branch"),
            P(),
            P(),
        ),
        out_specs=(P("col", "row", "branch"), P("row", "col", None)),
        check_vma=False,
    )
```
